8 devices in a mesh: dp: 2 (over y, z), sp: 4 (over x, core).
Axes of the slice: x: 2, y: 2, z: 1, core: 2. Of those that a mesh axis runs over, the one named last changes fastest.
Arguments:
- x: bfloat16 [4096, 3072], P(('dp', 'sp')), parts along dimension 0
- gain: bfloat16 [3072], replicated
- wq: bfloat16 [3072, 3072], replicated
- wk: bfloat16 [3072, 1024], replicated
- wv: bfloat16 [3072, 1024], replicated
- wo: bfloat16 [3072, 3072], replicated
Outputs:
- output: bfloat16 [4096, 3072], P(('dp', 'sp')), parts along dimension 0
There are 2 independent parts. The reference program is written for one: setup_inputs(seed, part) draws one part's arguments, and reference() takes and returns one part's arrays. A program takes and returns all parts, laid end to end along the dimension named above; an argument that names none is the same for every part.
All inputs are finite; a program needn't handle non-finite values.
Results may differ from the reference program's by a relative error of at most 0.012.
Values are sent between devices in bfloat16 or wider.
A program may use at most 2 GiB of HBM per device.

```python
import jax
import jax.numpy as jnp
from jax import lax

ROWS = 2048
D = 3072
HEADS = 24
KV_HEADS = 8
HEAD = 128
THETA = 10000


def setup_inputs(seed: int = 0, part: int = 0) -> dict:
    kx, kn, kq, kk, kv, ko = jax.random.split(jax.random.key(seed), 6)

    def weights(key, rows, columns):
        return jax.random.normal(key, (rows, columns), jnp.float32) * rows**-0.5

    drawn = {
        "x": jax.random.normal(jax.random.fold_in(kx, part), (ROWS, D), jnp.float32),
        "gain": 1 + 0.1 * jax.random.normal(kn, (D,), jnp.float32),
        "wq": 2 * weights(kq, D, HEADS * HEAD),
        "wk": 2 * weights(kk, D, KV_HEADS * HEAD),
        "wv": 4 * weights(kv, D, KV_HEADS * HEAD),
        "wo": weights(ko, HEADS * HEAD, D),
    }
    return {k: v.astype(jnp.bfloat16) for k, v in drawn.items()}


def normed(x, gain):
    wide = x.astype(jnp.float32)
    scale = lax.rsqrt(jnp.mean(wide * wide, -1, keepdims=True) + 1e-6)
    return (wide * scale * gain.astype(jnp.float32)).astype(jnp.bfloat16)


def turned(t, place, theta):
    half = t.shape[-1] // 2
    angle = place.astype(jnp.float32)[:, None] * theta ** (-jnp.arange(half, dtype=jnp.float32) / half)
    cos, sin = jnp.cos(angle)[:, None], jnp.sin(angle)[:, None]
    a, b = t[..., :half].astype(jnp.float32), t[..., half:].astype(jnp.float32)
    return jnp.concatenate([a * cos - b * sin, b * cos + a * sin], -1).astype(jnp.bfloat16)


def matmul(a, w):
    return jnp.dot(a, w, preferred_element_type=jnp.float32).astype(jnp.bfloat16)


def einsum(form, a, b):
    return jnp.einsum(form, a.astype(jnp.float32), b.astype(jnp.float32))


def attention(q, k, v):
    scores = einsum("tgsd,ugd->gstu", q, k) * q.shape[-1] ** -0.5
    token = jnp.arange(q.shape[0])
    scores = jnp.where(token[:, None] >= token, scores, -jnp.inf)
    weights = jax.nn.softmax(scores, -1).astype(jnp.bfloat16)
    return einsum("gstu,ugd->tgsd", weights, v).astype(jnp.bfloat16)


def reference(x, gain, wq, wk, wv, wo):
    a, place = normed(x, gain), jnp.arange(ROWS)
    q = turned(matmul(a, wq).reshape(ROWS, HEADS, HEAD), place, THETA).reshape(ROWS, KV_HEADS, -1, HEAD)
    k = turned(matmul(a, wk).reshape(ROWS, KV_HEADS, HEAD), place, THETA)
    v = matmul(a, wv).reshape(ROWS, KV_HEADS, HEAD)
    seen = attention(q, k, v).reshape(ROWS, HEADS * HEAD)
    return (x.astype(jnp.float32) + jnp.dot(seen, wo, preferred_element_type=jnp.float32)).astype(jnp.bfloat16)
```

```python
import functools

import jax
import jax.numpy as jnp
import numpy as np
from jax import lax
from jax.experimental import pallas as pl
from jax.experimental.pallas import tpu as pltpu
from jax.sharding import PartitionSpec as P

HEAD = 128
THETA = 10000
LOG2E = 1.4426950408889634
HIDDEN = -2e30
OWN = 512
D = 3072
KV = 8
HALF = 4
GROUP = 3
MINE = HALF * GROUP
WIDE = 256
TILES = 20
SLOTS = 4
BQ = 256
PAIRS = ((0, 0), (1, 0), (0, 2), (1, 2))


def dot(a, b, ca, cb):
    return lax.dot_general(a, b, (((ca,), (cb,)), ((), ())), preferred_element_type=jnp.float32)


def rope_table():
    half = HEAD // 2
    rate = np.float32(THETA) ** (-np.arange(half, dtype=np.float32) / np.float32(half))
    angle = np.arange(4 * OWN, dtype=np.float32)[:, None] * rate.astype(np.float32)
    cos, sin = np.cos(angle.astype(np.float64)), np.sin(angle.astype(np.float64))
    return np.concatenate([cos, cos, -sin, sin], -1).astype(np.float32)


def mixer(x_hbm, gain_ref, rope_hbm, wq, wk, wv, o_hbm, a_s, w_s, rope_s, kst, vst, qst, q_s, k_s, v_s, acc_s, top_s, sum_s, ob_s,
          in_sem, w_sem, own_sem, k_send, k_recv, v_send, v_recv, q_send, q_recv, f_send, f_recv, o_send, o_recv, oo_sem):
    me = lax.axis_index("sp")
    chip, core = lax.div(me, 2), lax.rem(me, 2)
    mate = 2 * chip + 1 - core
    e = HEAD**-0.5 * LOG2E

    def first_col(owner, head):
        return (owner * HALF + head) * HEAD

    def q_col(t):
        return lax.rem(t + MINE // 2 * (1 - core), MINE) * WIDE

    def tile_copy(src, col, slot):
        return pltpu.make_async_copy(src.at[:, pl.ds(pl.multiple_of(col, WIDE), WIDE)], w_s.at[slot], w_sem.at[slot])

    def kv_col(i):
        return lax.rem(i, 2) * (HALF * HEAD) + lax.div(i, 2) * WIDE

    load_x = pltpu.make_async_copy(x_hbm, a_s, in_sem.at[0])
    load_rope = pltpu.make_async_copy(rope_hbm.at[pl.ds(pl.multiple_of(me * OWN, OWN), OWN), :], rope_s, in_sem.at[1])
    load_x.start()
    load_rope.start()
    tile_copy(wk, 0, 0).start()
    tile_copy(wv, 0, 1).start()
    tile_copy(wk, kv_col(1), 2).start()
    tile_copy(wv, kv_col(1), 3).start()

    barrier = pltpu.get_barrier_semaphore()
    for step in (1, 2, 3):
        pl.semaphore_signal(barrier, inc=1, device_id={"sp": lax.rem(me + step, 4)}, device_id_type=pl.DeviceIdType.MESH)
    pl.semaphore_wait(barrier, 3)

    load_x.wait()
    gain = gain_ref[...].astype(jnp.float32)

    def norm(i, _):
        rows = pl.ds(pl.multiple_of(i * 32, 32), 32)
        wide = a_s[rows, :].astype(jnp.float32)
        scale = lax.rsqrt(jnp.mean(wide * wide, -1, keepdims=True) + 1e-6)
        a_s[rows, :] = (wide * scale * gain).astype(jnp.bfloat16)

    lax.fori_loop(0, OWN // 32, norm, None, unroll=2)
    load_rope.wait()

    def project(slot):
        return dot(a_s[...], w_s[slot], 1, 0)

    def turned(t):
        t = t.astype(jnp.bfloat16).astype(jnp.float32)
        return (t * rope_s[:, :HEAD] + pltpu.roll(t, HEAD // 2, 1) * rope_s[:, HEAD:]).astype(jnp.bfloat16)

    def remote(src, dst, send, recv, to):
        return pltpu.make_async_remote_copy(src_ref=src, dst_ref=dst, send_sem=send, recv_sem=recv, device_id={"sp": to},
                                            device_id_type=pl.DeviceIdType.MESH)

    def k_to_mate(j):
        return remote(kst.at[1 - core, j], k_s.at[me, j], k_send.at[j], k_recv.at[j], mate)

    def v_to_mate(j):
        return remote(vst.at[1 - core, j], v_s.at[me, j], v_send.at[j], v_recv.at[j], mate)

    def k_across(owner, j):
        return remote(kst.at[owner, j], k_s.at[me, j], f_send.at[0, owner, j], f_recv.at[0, me, j], 2 + owner)

    def v_across(owner, j):
        return remote(vst.at[owner, j], v_s.at[me, j], f_send.at[1, owner, j], f_recv.at[1, me, j], 2 + owner)

    def pair(i, _):
        owner, head = lax.rem(i, 2), 2 * lax.div(i, 2)
        slot = lax.rem(2 * i, SLOTS)
        tile_copy(wk, 0, slot).wait()
        k = project(slot)

        for n in range(2):
            kst[owner, head + n] = turned(k[:, n * HEAD : (n + 1) * HEAD])

        @pl.when(i < 2)
        def _():
            tile_copy(wk, kv_col(i + 2), slot).start()

        @pl.when(i >= 2)
        def _():
            tile_copy(wq, q_col(2 * (i - 2)), slot).start()

        tile_copy(wv, 0, slot + 1).wait()
        v = project(slot + 1)
        for n in range(2):
            vst[owner, head + n] = v[:, n * HEAD : (n + 1) * HEAD].astype(jnp.bfloat16).T

        @pl.when(i < 2)
        def _():
            tile_copy(wv, kv_col(i + 2), slot + 1).start()

        @pl.when(i >= 2)
        def _():
            tile_copy(wq, q_col(2 * (i - 2) + 1), slot + 1).start()

        @pl.when(chip == 0)
        def _():
            for n in range(2):
                k_across(owner, head + n).start()
                v_across(owner, head + n).start()

        @pl.when(owner != core)
        def _():
            for n in range(2):
                k_to_mate(head + n).start()
                v_to_mate(head + n).start()

    lax.fori_loop(0, 4, pair, None)
    own_k = pltpu.make_async_copy(kst.at[core], k_s.at[me], own_sem.at[0])
    own_v = pltpu.make_async_copy(vst.at[core], v_s.at[me], own_sem.at[1])
    own_k.start()
    own_v.start()

    mine = pl.ds(pl.multiple_of(core * OWN, OWN), OWN)

    def q_to_mate(t):
        two = pl.ds(2 * t, 2)
        return remote(qst.at[two], q_s.at[two, mine, :], q_send.at[t], q_recv.at[t], mate)

    def query(t, _):
        slot = lax.rem(t, SLOTS)
        tile_copy(wq, 0, slot).wait()
        q = project(slot)

        @pl.when(t < MINE - SLOTS)
        def _():
            tile_copy(wq, q_col(t + SLOTS), slot).start()

        @pl.when(t < MINE // 2)
        def _():
            for n in range(2):
                qst[2 * t + n] = turned(q[:, n * HEAD : (n + 1) * HEAD])
            q_to_mate(t).start()

        @pl.when(t >= MINE // 2)
        def _():
            for n in range(2):
                q_s[2 * t - MINE + n, mine, :] = turned(q[:, n * HEAD : (n + 1) * HEAD])

    lax.fori_loop(0, MINE, query, None)

    own_k.wait()
    own_v.wait()
    for j in range(HALF):
        k_to_mate(j).wait()
        v_to_mate(j).wait()
    for t in range(MINE // 2):
        q_to_mate(t).wait()

    hidden = lax.broadcasted_iota(jnp.int32, (BQ, BQ), 0) > lax.broadcasted_iota(jnp.int32, (BQ, BQ), 1)

    def soften(parts):
        top = functools.reduce(jnp.maximum, [s.max(axis=0, keepdims=True) for s in parts])
        weights = [jnp.exp2((s - top) * e) for s in parts]
        total = functools.reduce(jnp.add, [p.sum(axis=0, keepdims=True) for p in weights])
        return jnp.concatenate([p.astype(jnp.bfloat16) for p in weights], axis=0), top, total

    def o_to_mate(j):
        return remote(ob_s.at[1 - core, j], o_hbm.at[:, pl.ds(pl.multiple_of((core * HALF + j) * GROUP * HEAD, HEAD), GROUP * HEAD)],
                      o_send.at[j], o_recv.at[j], mate)

    def o_home(j):
        return pltpu.make_async_copy(ob_s.at[core, j], o_hbm.at[:, pl.ds(pl.multiple_of((core * HALF + j) * GROUP * HEAD, HEAD), GROUP * HEAD)],
                                     oo_sem.at[j])

    def finish(j, r, b, o, total):
        rows = (b % 2) * BQ
        ob_s[b // 2, j, rows : rows + BQ, r * HEAD : (r + 1) * HEAD] = (o * (1 / total)).T.astype(jnp.bfloat16)

    def near(j, last):
        for b in range(2 * OWN // BQ):
            for r in range(GROUP):
                q = q_s[j * GROUP + r, b * BQ : (b + 1) * BQ, :]
                parts, values = [], []
                for n in range(b + 1):
                    block, row = 2 * chip + n * BQ // OWN, n * BQ % OWN
                    s = dot(k_s[block, j, row : row + BQ, :], q, 1, 1)
                    parts.append(jnp.where(hidden, HIDDEN, s) if n == b else s)
                    values.append(v_s[block, j, :, row : row + BQ])
                p, top, total = soften(parts)
                o = dot(jnp.concatenate(values, axis=1), p, 1, 0)
                if last:
                    finish(j, r, b, o, total)
                else:
                    here = slice(b * BQ, (b + 1) * BQ)
                    acc_s[j * GROUP + r, :, here] = o
                    top_s[j * GROUP + r, :, here] = top
                    sum_s[j * GROUP + r, :, here] = total

    def far(j):
        for b in range(2 * OWN // BQ):
            for r in range(GROUP):
                q = q_s[j * GROUP + r, b * BQ : (b + 1) * BQ, :]
                here = slice(b * BQ, (b + 1) * BQ)
                parts = [dot(k_s[n, j], q, 1, 1) for n in range(2)]
                p, top, total = soften(parts)
                o = dot(jnp.concatenate([v_s[0, j], v_s[1, j]], axis=1), p, 1, 0)
                old = top_s[j * GROUP + r, :, here]
                new = jnp.maximum(old, top)
                a, c = jnp.exp2((old - new) * e), jnp.exp2((top - new) * e)
                finish(j, r, b, acc_s[j * GROUP + r, :, here] * a + o * c, sum_s[j * GROUP + r, :, here] * a + total * c)

    @pl.when(chip == 0)
    def _():
        def step(j, _):
            near(j, True)
            o_to_mate(j).start()
            o_home(j).start()

        lax.fori_loop(0, HALF, step, None)
        for owner in range(2):
            for j in range(HALF):
                k_across(owner, j).wait_send()
                v_across(owner, j).wait_send()

    @pl.when(chip == 1)
    def _():
        lax.fori_loop(0, HALF, lambda j, _: near(j, False), None)

        def step(j, _):
            for n in range(2):
                remote(kst.at[0, 0], k_s.at[n, j], f_send.at[0, 0, 0], f_recv.at[0, n, j], 0).wait_recv()
                remote(vst.at[0, 0], v_s.at[n, j], f_send.at[1, 0, 0], f_recv.at[1, n, j], 0).wait_recv()
            far(j)
            o_to_mate(j).start()
            o_home(j).start()

        lax.fori_loop(0, HALF, step, None)

    for j in range(HALF):
        o_to_mate(j).wait()
        o_home(j).wait()


def attended(x, gain, wq, wk, wv):
    dma = pltpu.SemaphoreType.DMA
    bf, f32 = jnp.bfloat16, jnp.float32
    anywhere = pl.BlockSpec(memory_space=pl.ANY)
    return pl.pallas_call(
        mixer,
        out_shape=jax.ShapeDtypeStruct((OWN, D), bf),
        in_specs=[anywhere, pl.BlockSpec(memory_space=pltpu.VMEM), anywhere, anywhere, anywhere, anywhere],
        out_specs=anywhere,
        scratch_shapes=[
            pltpu.VMEM((OWN, D), bf),
            pltpu.VMEM((SLOTS, D, WIDE), bf),
            pltpu.VMEM((OWN, 2 * HEAD), f32),
            pltpu.VMEM((2, HALF, OWN, HEAD), bf),
            pltpu.VMEM((2, HALF, HEAD, OWN), bf),
            pltpu.VMEM((MINE, OWN, HEAD), bf),
            pltpu.VMEM((MINE, 2 * OWN, HEAD), bf),
            pltpu.VMEM((4, HALF, OWN, HEAD), bf),
            pltpu.VMEM((4, HALF, HEAD, OWN), bf),
            pltpu.VMEM((MINE, HEAD, 2 * OWN), f32),
            pltpu.VMEM((MINE, 1, 2 * OWN), f32),
            pltpu.VMEM((MINE, 1, 2 * OWN), f32),
            pltpu.VMEM((2, HALF, OWN, GROUP * HEAD), bf),
            dma((2,)), dma((SLOTS,)), dma((2,)),
            dma((HALF,)), dma((HALF,)), dma((HALF,)), dma((HALF,)),
            dma((MINE // 2,)), dma((MINE // 2,)),
            dma((2, 2, HALF)), dma((2, 2, HALF)),
            dma((HALF,)), dma((HALF,)), dma((HALF,)),
        ],
        compiler_params=pltpu.CompilerParams(collective_id=0, has_side_effects=True, vmem_limit_bytes=60 * 2**20),
        cost_estimate=pl.CostEstimate(flops=30 * 10**9, bytes_accessed=40 * 2**20, transcendentals=20 * 10**6),
    )(x, gain, jnp.asarray(rope_table()), wq, wk, wv)


def closing(x_ref, o_ref, w_ref, y_ref):
    y = dot(o_ref[...], w_ref[...], 1, 0)
    y_ref[...] = (x_ref[...].astype(jnp.float32) + y).astype(jnp.bfloat16)


def closed(x, o, wo):
    return pl.pallas_call(
        closing,
        grid=(D // WIDE,),
        out_shape=jax.ShapeDtypeStruct((OWN, D), jnp.bfloat16),
        in_specs=[pl.BlockSpec((OWN, WIDE), lambda i: (0, i)), pl.BlockSpec((OWN, D), lambda i: (0, 0)), pl.BlockSpec((D, WIDE), lambda i: (0, i))],
        out_specs=pl.BlockSpec((OWN, WIDE), lambda i: (0, i)),
        compiler_params=pltpu.CompilerParams(vmem_limit_bytes=40 * 2**20),
        cost_estimate=pl.CostEstimate(flops=2 * OWN * D * D, bytes_accessed=2 * D * D + 6 * OWN * D, transcendentals=0),
    )(x, o, wo)


def solution(mesh):
    def step(x, gain, wq, wk, wv, wo):
        return closed(x, attended(x, gain[None], wq, wk, wv), wo)

    tokens, whole = P(("dp", "sp"), None), P(None, None)
    return jax.shard_map(
        step,
        mesh=mesh,
        in_specs=(tokens, P(None), whole, whole, whole, whole),
        out_specs=tokens,
        check_vma=False,
    )
```

```python
import functools

import jax
import jax.numpy as jnp
import numpy as np
from jax import lax
from jax.experimental import pallas as pl
from jax.experimental.pallas import tpu as pltpu
from jax.sharding import PartitionSpec as P

HEAD = 128
THETA = 10000
LOG2E = 1.4426950408889634
HIDDEN = -2e30
OWN = 512
D = 3072
KV = 8
HALF = 4
GROUP = 3
MINE = HALF * GROUP
WIDE = 512
Q_TILES = 6
SLOTS = 3
BQ = 256
CHUNK = 256
LEAD = 4
RING = 8


def dot(a, b, ca, cb):
    return lax.dot_general(a, b, (((ca,), (cb,)), ((), ())), preferred_element_type=jnp.float32)


def rope_table():
    half = HEAD // 2
    rate = np.float32(THETA) ** (-np.arange(half, dtype=np.float32) / np.float32(half))
    angle = np.arange(4 * OWN, dtype=np.float32)[:, None] * rate.astype(np.float32)
    return np.concatenate([np.cos(angle.astype(np.float64)), np.sin(angle.astype(np.float64))], -1).astype(np.float32)


def mixer(x_hbm, gain_ref, rope_hbm, wq, wk, wv, o_hbm, a_s, w_s, rope_s, kst, vst, q_s, k_s, v_s, s_s, acc_s, top_s, sum_s, ob_s,
          in_sem, w_sem, own_sem, k_send, k_recv, v_send, v_recv, q_send, q_recv, f_send, f_recv, o_send, o_recv, oo_sem):
    me = lax.axis_index("sp")
    chip, core = lax.div(me, 2), lax.rem(me, 2)
    mate = 2 * chip + 1 - core
    e = HEAD**-0.5 * LOG2E

    def kv_copies(i, slot):
        col = pl.ds(pl.multiple_of(lax.rem(i, 2) * (HALF * HEAD) + lax.div(i, 2) * (WIDE // 2), WIDE // 2), WIDE // 2)
        return (pltpu.make_async_copy(wk.at[:, col], w_s.at[slot, :, : WIDE // 2], w_sem.at[slot, 0]),
                pltpu.make_async_copy(wv.at[:, col], w_s.at[slot, :, WIDE // 2 :], w_sem.at[slot, 1]))

    def q_copy(t, slot):
        col = pl.multiple_of(lax.rem(t + Q_TILES // 2 * (1 - core), Q_TILES) * WIDE, WIDE)
        return pltpu.make_async_copy(wq.at[:, pl.ds(col, WIDE)], w_s.at[slot], w_sem.at[slot, 0])

    load_x = pltpu.make_async_copy(x_hbm, a_s, in_sem.at[0])
    load_rope = pltpu.make_async_copy(rope_hbm.at[pl.ds(pl.multiple_of(me * OWN, OWN), OWN), :], rope_s.at[:, :HEAD], in_sem.at[1])
    load_x.start()
    load_rope.start()
    for n in range(SLOTS):
        for copy in kv_copies(n, n):
            copy.start()

    barrier = pltpu.get_barrier_semaphore()
    for step in (1, 2, 3):
        pl.semaphore_signal(barrier, inc=1, device_id={"sp": lax.rem(me + step, 4)}, device_id_type=pl.DeviceIdType.MESH)
    pl.semaphore_wait(barrier, 3)

    load_rope.wait()
    table = rope_s[:, :HEAD]
    swapped = pltpu.roll(table, HEAD // 2, 1)
    low = lax.broadcasted_iota(jnp.int32, (OWN, HEAD), 1) < HEAD // 2
    rope_s[:, :HEAD] = jnp.where(low, table, swapped)
    rope_s[:, HEAD:] = jnp.where(low, -swapped, table)
    load_x.wait()
    gain = gain_ref[...].astype(jnp.float32)[None]

    def norm(i, _):
        rows = pl.ds(pl.multiple_of(i * 32, 32), 32)
        wide = a_s[rows, :].astype(jnp.float32)
        scale = lax.rsqrt(jnp.mean(wide * wide, -1, keepdims=True) + 1e-6)
        a_s[rows, :] = (wide * scale * gain).astype(jnp.bfloat16)

    lax.fori_loop(0, OWN // 32, norm, None, unroll=2)

    def turned(t):
        t = t.astype(jnp.bfloat16).astype(jnp.float32)
        return (t * rope_s[:, :HEAD] + pltpu.roll(t, HEAD // 2, 1) * rope_s[:, HEAD:]).astype(jnp.bfloat16)

    def remote(src, dst, send, recv, to):
        return pltpu.make_async_remote_copy(src_ref=src, dst_ref=dst, send_sem=send, recv_sem=recv, device_id={"sp": to},
                                            device_id_type=pl.DeviceIdType.MESH)

    def k_to_mate(j):
        return remote(kst.at[1 - core, j], k_s.at[me, j], k_send.at[j], k_recv.at[j], mate)

    def v_to_mate(j):
        return remote(vst.at[1 - core, j], v_s.at[me, j], v_send.at[j], v_recv.at[j], mate)

    def k_across(owner, j):
        return remote(kst.at[owner, j], k_s.at[me, j], f_send.at[0, owner, j], f_recv.at[0, me, j], 2 + owner)

    def v_across(owner, j):
        return remote(vst.at[owner, j], v_s.at[me, j], f_send.at[1, owner, j], f_recv.at[1, me, j], 2 + owner)

    def pair(i, _):
        owner, head = lax.rem(i, 2), 2 * lax.div(i, 2)
        slot = lax.rem(i, SLOTS)
        for copy in kv_copies(i, slot):
            copy.wait()
        kv = dot(a_s[...], w_s[slot], 1, 0)
        for n in range(2):
            kst[owner, head + n] = turned(kv[:, n * HEAD : (n + 1) * HEAD])
            vst[owner, head + n] = kv[:, (n + 2) * HEAD : (n + 3) * HEAD].astype(jnp.bfloat16).T

        @pl.when(i + SLOTS < 4)
        def _():
            for copy in kv_copies(i + SLOTS, slot):
                copy.start()

        @pl.when(i + SLOTS >= 4)
        def _():
            q_copy(i + SLOTS - 4, slot).start()

        def send(owner, j):
            k_across(owner, j).start()
            v_across(owner, j).start()

        @pl.when((chip == 0) & (owner == 0))
        def _():
            send(0, head)

        @pl.when((chip == 0) & (owner == 1))
        def _():
            send(1, head)
            send(0, head + 1)
            send(1, head + 1)

        @pl.when(owner != core)
        def _():
            for n in range(2):
                k_to_mate(head + n).start()
                v_to_mate(head + n).start()

    lax.fori_loop(0, 4, pair, None)
    own_k = pltpu.make_async_copy(kst.at[core], k_s.at[me], own_sem.at[0])
    own_v = pltpu.make_async_copy(vst.at[core], v_s.at[me], own_sem.at[1])
    own_k.start()
    own_v.start()

    def q_to_mate(t):
        four = pl.ds(4 * t, 4)
        return remote(q_s.at[0, four], q_s.at[1 + core, four], q_send.at[t], q_recv.at[t], mate)

    def query(t, _):
        slot = lax.rem(t + 4, SLOTS)
        q_copy(t, slot).wait()
        q = dot(a_s[...], w_s[slot], 1, 0)
        away = t < Q_TILES // 2
        place, head = jnp.where(away, 0, 1 + core), 4 * jnp.where(away, t, t - Q_TILES // 2)
        for n in range(4):
            q_s[place, head + n] = turned(q[:, n * HEAD : (n + 1) * HEAD])

        @pl.when(t < Q_TILES - SLOTS)
        def _():
            q_copy(t + SLOTS, slot).start()

        @pl.when(away)
        def _():
            q_to_mate(t).start()

    lax.fori_loop(0, Q_TILES, query, None)

    own_k.wait()
    own_v.wait()
    for j in range(HALF):
        k_to_mate(j).wait()
        v_to_mate(j).wait()
    for t in range(Q_TILES // 2):
        q_to_mate(t).wait()

    def attend(blocks):
        chunks = [(i, n) for i, (_, parts, _) in enumerate(blocks) for n in range(len(parts))]
        tops = {}

        def score(g):
            if g >= len(chunks):
                return
            i, n = chunks[g]
            queries, parts, _ = blocks[i]
            keys, _, masked = parts[n]
            s = dot(keys(), queries(), 1, 1)
            if masked:
                s = jnp.where(lax.broadcasted_iota(jnp.int32, s.shape, 0) > lax.broadcasted_iota(jnp.int32, s.shape, 1), HIDDEN, s)
            s_s[g % RING] = s
            top = s.reshape(CHUNK // 8, 8, BQ).max(axis=0)
            tops[i] = jnp.maximum(tops[i], top) if i in tops else top

        for g in range(LEAD):
            score(g)
        g = 0
        for i, (_, parts, sink) in enumerate(blocks):
            top = tops[i].max(axis=0, keepdims=True) * e
            out = total = None
            for _, values, _ in parts:
                score(g + LEAD)
                p = jnp.exp2(s_s[g % RING] * e - top)
                t = p.reshape(CHUNK // 8, 8, BQ).sum(axis=0)
                o = dot(values(), p.astype(jnp.bfloat16), 1, 0)
                out, total = (o, t) if out is None else (out + o, total + t)
                g += 1
            sink(out, top, total.sum(axis=0, keepdims=True))

    def key(block, j, row):
        return lambda: k_s[block, j, row : row + CHUNK, :]

    def value(block, j, row):
        return lambda: v_s[block, j, :, row : row + CHUNK]

    def queries(j, r, b):
        return lambda: q_s[1 + b * BQ // OWN, j * GROUP + r, b * BQ % OWN : b * BQ % OWN + BQ, :]

    def o_cols(j):
        return pl.ds(pl.multiple_of((core * HALF + j) * GROUP * HEAD, HEAD), GROUP * HEAD)

    def o_to_mate(j):
        return remote(ob_s.at[1 - core, j], o_hbm.at[:, o_cols(j)], o_send.at[j], o_recv.at[j], mate)

    def o_home(j):
        return pltpu.make_async_copy(ob_s.at[core, j], o_hbm.at[:, o_cols(j)], oo_sem.at[j])

    def finish(j, r, b, o, total):
        rows = b * BQ % OWN
        ob_s[b * BQ // OWN, j, rows : rows + BQ, r * HEAD : (r + 1) * HEAD] = (o * (1 / total)).T.astype(jnp.bfloat16)

    def near(j, last):
        def block(b, r):
            parts = []
            for n in range(b + 1):
                at = 2 * chip + n * CHUNK // OWN, j, n * CHUNK % OWN
                parts.append((key(*at), value(*at), n == b))

            def sink(o, top, total):
                if last:
                    finish(j, r, b, o, total)
                else:
                    here = slice(b * BQ, (b + 1) * BQ)
                    acc_s[j * GROUP + r, :, here] = o
                    top_s[j * GROUP + r, :, here] = top
                    sum_s[j * GROUP + r, :, here] = total

            return queries(j, r, b), parts, sink

        attend([block(b, r) for b in range(2 * OWN // BQ) for r in range(GROUP)])

    def far(j):
        def block(b, r):
            parts = [(key(n * CHUNK // OWN, j, n * CHUNK % OWN), value(n * CHUNK // OWN, j, n * CHUNK % OWN), False) for n in range(2 * OWN // CHUNK)]

            def sink(o, top, total):
                here = slice(b * BQ, (b + 1) * BQ)
                old = top_s[j * GROUP + r, :, here]
                new = jnp.maximum(old, top)
                a, c = jnp.exp2(old - new), jnp.exp2(top - new)
                finish(j, r, b, acc_s[j * GROUP + r, :, here] * a + o * c, sum_s[j * GROUP + r, :, here] * a + total * c)

            return queries(j, r, b), parts, sink

        attend([block(b, r) for b in range(2 * OWN // BQ) for r in range(GROUP)])

    @pl.when(chip == 0)
    def _():
        def step(j, _):
            near(j, True)
            o_to_mate(j).start()
            o_home(j).start()

        lax.fori_loop(0, HALF, step, None)
        for owner in range(2):
            for j in range(HALF):
                k_across(owner, j).wait_send()
                v_across(owner, j).wait_send()

    @pl.when(chip == 1)
    def _():
        lax.fori_loop(0, HALF, lambda j, _: near(j, False), None)

        def step(j, _):
            for n in range(2):
                remote(kst.at[0, 0], k_s.at[n, j], f_send.at[0, 0, 0], f_recv.at[0, n, j], 0).wait_recv()
                remote(vst.at[0, 0], v_s.at[n, j], f_send.at[1, 0, 0], f_recv.at[1, n, j], 0).wait_recv()
            far(j)
            o_to_mate(j).start()
            o_home(j).start()

        lax.fori_loop(0, HALF, step, None)

    for j in range(HALF):
        o_to_mate(j).wait()
        o_home(j).wait()


def attended(x, gain, wq, wk, wv):
    dma = pltpu.SemaphoreType.DMA
    bf, f32 = jnp.bfloat16, jnp.float32
    anywhere = pl.BlockSpec(memory_space=pl.ANY)
    return pl.pallas_call(
        mixer,
        out_shape=jax.ShapeDtypeStruct((OWN, D), bf),
        in_specs=[anywhere, pl.BlockSpec(memory_space=pltpu.VMEM), anywhere, anywhere, anywhere, anywhere],
        out_specs=anywhere,
        scratch_shapes=[
            pltpu.VMEM((OWN, D), bf),
            pltpu.VMEM((SLOTS, D, WIDE), bf),
            pltpu.VMEM((OWN, 2 * HEAD), f32),
            pltpu.VMEM((2, HALF, OWN, HEAD), bf),
            pltpu.VMEM((2, HALF, HEAD, OWN), bf),
            pltpu.VMEM((3, MINE, OWN, HEAD), bf),
            pltpu.VMEM((4, HALF, OWN, HEAD), bf),
            pltpu.VMEM((4, HALF, HEAD, OWN), bf),
            pltpu.VMEM((RING, CHUNK, BQ), f32),
            pltpu.VMEM((MINE, HEAD, 2 * OWN), f32),
            pltpu.VMEM((MINE, 1, 2 * OWN), f32),
            pltpu.VMEM((MINE, 1, 2 * OWN), f32),
            pltpu.VMEM((2, HALF, OWN, GROUP * HEAD), bf),
            dma((2,)), dma((SLOTS, 2)), dma((2,)),
            dma((HALF,)), dma((HALF,)), dma((HALF,)), dma((HALF,)),
            dma((Q_TILES // 2,)), dma((Q_TILES // 2,)),
            dma((2, 2, HALF)), dma((2, 2, HALF)),
            dma((HALF,)), dma((HALF,)), dma((HALF,)),
        ],
        compiler_params=pltpu.CompilerParams(collective_id=0, has_side_effects=True, vmem_limit_bytes=60 * 2**20),
        cost_estimate=pl.CostEstimate(flops=30 * 10**9, bytes_accessed=40 * 2**20, transcendentals=20 * 10**6),
    )(x, gain, jnp.asarray(rope_table()), wq, wk, wv)


def closing(x_ref, o_ref, w_ref, y_ref):
    y = dot(o_ref[...], w_ref[...], 1, 0)
    y_ref[...] = (x_ref[...].astype(jnp.float32) + y).astype(jnp.bfloat16)


def closed(x, o, wo):
    return pl.pallas_call(
        closing,
        grid=(D // WIDE,),
        out_shape=jax.ShapeDtypeStruct((OWN, D), jnp.bfloat16),
        in_specs=[pl.BlockSpec((OWN, WIDE), lambda i: (0, i)), pl.BlockSpec((OWN, D), lambda i: (0, 0)), pl.BlockSpec((D, WIDE), lambda i: (0, i))],
        out_specs=pl.BlockSpec((OWN, WIDE), lambda i: (0, i)),
        compiler_params=pltpu.CompilerParams(vmem_limit_bytes=56 * 2**20),
        cost_estimate=pl.CostEstimate(flops=2 * OWN * D * D, bytes_accessed=2 * D * D + 6 * OWN * D, transcendentals=0),
    )(x, o, wo)


def solution(mesh):
    def step(x, gain, wq, wk, wv, wo):
        return closed(x, attended(x, gain, wq, wk, wv), wo)

    tokens, whole = P(("dp", "sp"), None), P(None, None)
    return jax.shard_map(
        step,
        mesh=mesh,
        in_specs=(tokens, P(None), whole, whole, whole, whole),
        out_specs=tokens,
        check_vma=False,
    )
```

```python
import functools

import jax
import jax.numpy as jnp
import numpy as np
from jax import lax
from jax.experimental import pallas as pl
from jax.experimental.pallas import tpu as pltpu
from jax.sharding import PartitionSpec as P

HEAD = 128
THETA = 10000
LOG2E = 1.4426950408889634
HIDDEN = -2e30
OWN = 512
D = 3072
KV = 8
HALF = 4
GROUP = 3
MINE = HALF * GROUP
WIDE = 512
Q_TILES = 6
SLOTS = 3
BQ = 256
CHUNK = 256
LEAD = 4
RING = 8


def dot(a, b, ca, cb):
    return lax.dot_general(a, b, (((ca,), (cb,)), ((), ())), preferred_element_type=jnp.float32)


def rope_table():
    half = HEAD // 2
    rate = np.float32(THETA) ** (-np.arange(half, dtype=np.float32) / np.float32(half))
    angle = np.arange(4 * OWN, dtype=np.float32)[:, None] * rate.astype(np.float32)
    return np.concatenate([np.cos(angle.astype(np.float64)), np.sin(angle.astype(np.float64))], -1).astype(np.float32)


def mixer(x_hbm, gain_ref, rope_hbm, wq, wk, wv, wo, y_hbm, a_s, w_s, rope_s, kst, vst, q_s, k_s, v_s, s_s, acc_s, top_s, sum_s, o_s, wo_s, y_s,
          in_sem, w_sem, own_sem, k_send, k_recv, v_send, v_recv, q_send, q_recv, f_send, f_recv, o_send, o_recv, wo_sem, y_sem):
    me = lax.axis_index("sp")
    chip, core = lax.div(me, 2), lax.rem(me, 2)
    mate = 2 * chip + 1 - core
    e = HEAD**-0.5 * LOG2E

    def kv_copies(i, slot):
        col = pl.ds(pl.multiple_of(lax.rem(i, 2) * (HALF * HEAD) + lax.div(i, 2) * (WIDE // 2), WIDE // 2), WIDE // 2)
        return (pltpu.make_async_copy(wk.at[:, col], w_s.at[slot, :, : WIDE // 2], w_sem.at[slot, 0]),
                pltpu.make_async_copy(wv.at[:, col], w_s.at[slot, :, WIDE // 2 :], w_sem.at[slot, 1]))

    def q_copy(t, slot):
        col = pl.multiple_of(lax.rem(t + Q_TILES // 2 * (1 - core), Q_TILES) * WIDE, WIDE)
        return pltpu.make_async_copy(wq.at[:, pl.ds(col, WIDE)], w_s.at[slot], w_sem.at[slot, 0])

    load_x = pltpu.make_async_copy(x_hbm, a_s, in_sem.at[0])
    load_rope = pltpu.make_async_copy(rope_hbm.at[pl.ds(pl.multiple_of(me * OWN, OWN), OWN), :], rope_s.at[:, :HEAD], in_sem.at[1])
    load_x.start()
    load_rope.start()
    for n in range(SLOTS):
        for copy in kv_copies(n, n):
            copy.start()

    barrier = pltpu.get_barrier_semaphore()
    for step in (1, 2, 3):
        pl.semaphore_signal(barrier, inc=1, device_id={"sp": lax.rem(me + step, 4)}, device_id_type=pl.DeviceIdType.MESH)
    pl.semaphore_wait(barrier, 3)

    load_rope.wait()
    table = rope_s[:, :HEAD]
    swapped = pltpu.roll(table, HEAD // 2, 1)
    low = lax.broadcasted_iota(jnp.int32, (OWN, HEAD), 1) < HEAD // 2
    rope_s[:, :HEAD] = jnp.where(low, table, swapped)
    rope_s[:, HEAD:] = jnp.where(low, -swapped, table)
    load_x.wait()
    gain = gain_ref[...].astype(jnp.float32)[None]

    def norm(i, _):
        rows = pl.ds(pl.multiple_of(i * 32, 32), 32)
        wide = a_s[rows, :].astype(jnp.float32)
        scale = lax.rsqrt(jnp.mean(wide * wide, -1, keepdims=True) + 1e-6)
        a_s[rows, :] = (wide * scale * gain).astype(jnp.bfloat16)
        y_s[rows, :] = wide

    lax.fori_loop(0, OWN // 32, norm, None, unroll=2)

    def turned(t):
        t = t.astype(jnp.bfloat16).astype(jnp.float32)
        return (t * rope_s[:, :HEAD] + pltpu.roll(t, HEAD // 2, 1) * rope_s[:, HEAD:]).astype(jnp.bfloat16)

    def remote(src, dst, send, recv, to):
        return pltpu.make_async_remote_copy(src_ref=src, dst_ref=dst, send_sem=send, recv_sem=recv, device_id={"sp": to},
                                            device_id_type=pl.DeviceIdType.MESH)

    def k_to_mate(j):
        return remote(kst.at[1 - core, j], k_s.at[me, j], k_send.at[j], k_recv.at[j], mate)

    def v_to_mate(j):
        return remote(vst.at[1 - core, j], v_s.at[me, j], v_send.at[j], v_recv.at[j], mate)

    def k_across(owner, j):
        return remote(kst.at[owner, j], k_s.at[me, j], f_send.at[0, owner, j], f_recv.at[0, me, j], 2 + owner)

    def v_across(owner, j):
        return remote(vst.at[owner, j], v_s.at[me, j], f_send.at[1, owner, j], f_recv.at[1, me, j], 2 + owner)

    def pair(i, _):
        owner, head = lax.rem(i, 2), 2 * lax.div(i, 2)
        slot = lax.rem(i, SLOTS)
        for copy in kv_copies(i, slot):
            copy.wait()
        kv = dot(a_s[...], w_s[slot], 1, 0)
        for n in range(2):
            kst[owner, head + n] = turned(kv[:, n * HEAD : (n + 1) * HEAD])
            vst[owner, head + n] = kv[:, (n + 2) * HEAD : (n + 3) * HEAD].astype(jnp.bfloat16).T

        @pl.when(i + SLOTS < 4)
        def _():
            for copy in kv_copies(i + SLOTS, slot):
                copy.start()

        @pl.when(i + SLOTS >= 4)
        def _():
            q_copy(i + SLOTS - 4, slot).start()

        def send(owner, j):
            k_across(owner, j).start()
            v_across(owner, j).start()

        @pl.when((chip == 0) & (owner == 0))
        def _():
            send(0, head)

        @pl.when((chip == 0) & (owner == 1))
        def _():
            send(1, head)
            send(0, head + 1)
            send(1, head + 1)

        @pl.when(owner != core)
        def _():
            for n in range(2):
                k_to_mate(head + n).start()
                v_to_mate(head + n).start()

    lax.fori_loop(0, 4, pair, None)
    own_k = pltpu.make_async_copy(kst.at[core], k_s.at[me], own_sem.at[0])
    own_v = pltpu.make_async_copy(vst.at[core], v_s.at[me], own_sem.at[1])
    own_k.start()
    own_v.start()

    def q_to_mate(t):
        four = pl.ds(4 * t, 4)
        return remote(q_s.at[0, four], q_s.at[1 + core, four], q_send.at[t], q_recv.at[t], mate)

    def query(t, _):
        slot = lax.rem(t + 4, SLOTS)
        q_copy(t, slot).wait()
        q = dot(a_s[...], w_s[slot], 1, 0)
        away = t < Q_TILES // 2
        place, head = jnp.where(away, 0, 1 + core), 4 * jnp.where(away, t, t - Q_TILES // 2)
        for n in range(4):
            q_s[place, head + n] = turned(q[:, n * HEAD : (n + 1) * HEAD])

        @pl.when(t < Q_TILES - SLOTS)
        def _():
            q_copy(t + SLOTS, slot).start()

        @pl.when(away)
        def _():
            q_to_mate(t).start()

    lax.fori_loop(0, Q_TILES, query, None)

    RUN = GROUP * HEAD

    def wo_copies(j):
        slot = lax.rem(j, 2)
        return tuple(pltpu.make_async_copy(wo.at[pl.ds(pl.multiple_of((owner * HALF + j) * RUN, RUN), RUN), :],
                                           wo_s.at[slot, n * RUN : (n + 1) * RUN], wo_sem.at[slot, n])
                     for n, owner in enumerate((core, 1 - core)))

    def y_copy(n):
        return pltpu.make_async_copy(a_s.at[:, n * WIDE : (n + 1) * WIDE], y_hbm.at[:, n * WIDE : (n + 1) * WIDE], y_sem.at[n])

    for j in range(2):
        for copy in wo_copies(j):
            copy.start()

    def close(j, last=False):
        for copy in wo_copies(j):
            copy.wait()
        o_to_mate(j).wait()
        slot = lax.rem(j, 2)
        for n in range(D // WIDE):
            here = slice(n * WIDE, (n + 1) * WIDE)
            y = y_s[:, here] + dot(o_s[core, j], wo_s[slot, :, here], 1, 0)
            if last:
                a_s[:, here] = y.astype(jnp.bfloat16)
                y_copy(n).start()
            else:
                y_s[:, here] = y

    own_k.wait()
    own_v.wait()
    for j in range(HALF):
        k_to_mate(j).wait()
        v_to_mate(j).wait()
    for t in range(Q_TILES // 2):
        q_to_mate(t).wait()

    def attend(blocks):
        chunks = [(i, n) for i, (_, parts, _) in enumerate(blocks) for n in range(len(parts))]
        tops = {}

        def score(g):
            if g >= len(chunks):
                return
            i, n = chunks[g]
            queries, parts, _ = blocks[i]
            keys, _, masked = parts[n]
            s = dot(keys(), queries(), 1, 1)
            if masked:
                s = jnp.where(lax.broadcasted_iota(jnp.int32, s.shape, 0) > lax.broadcasted_iota(jnp.int32, s.shape, 1), HIDDEN, s)
            s_s[g % RING] = s
            top = s.reshape(CHUNK // 8, 8, BQ).max(axis=0)
            tops[i] = jnp.maximum(tops[i], top) if i in tops else top

        for g in range(LEAD):
            score(g)
        g = 0
        for i, (_, parts, sink) in enumerate(blocks):
            top = tops[i].max(axis=0, keepdims=True) * e
            out = total = None
            for _, values, _ in parts:
                score(g + LEAD)
                p = jnp.exp2(s_s[g % RING] * e - top)
                t = p.reshape(CHUNK // 8, 8, BQ).sum(axis=0)
                o = dot(values(), p.astype(jnp.bfloat16), 1, 0)
                out, total = (o, t) if out is None else (out + o, total + t)
                g += 1
            sink(out, top, total.sum(axis=0, keepdims=True))

    def key(block, j, row):
        return lambda: k_s[block, j, row : row + CHUNK, :]

    def value(block, j, row):
        return lambda: v_s[block, j, :, row : row + CHUNK]

    def queries(j, r, b):
        return lambda: q_s[1 + b * BQ // OWN, j * GROUP + r, b * BQ % OWN : b * BQ % OWN + BQ, :]

    def o_to_mate(j):
        return remote(o_s.at[1 - core, j, :, :RUN], o_s.at[1 - core, j, :, RUN:], o_send.at[j], o_recv.at[j], mate)

    def finish(j, r, b, o, total):
        rows = b * BQ % OWN
        o_s[b * BQ // OWN, j, rows : rows + BQ, r * HEAD : (r + 1) * HEAD] = (o * (1 / total)).T.astype(jnp.bfloat16)

    def near(j, last):
        def block(b, r):
            parts = []
            for n in range(b + 1):
                at = 2 * chip + n * CHUNK // OWN, j, n * CHUNK % OWN
                parts.append((key(*at), value(*at), n == b))

            def sink(o, top, total):
                if last:
                    finish(j, r, b, o, total)
                else:
                    here = slice(b * BQ, (b + 1) * BQ)
                    acc_s[j * GROUP + r, :, here] = o
                    top_s[j * GROUP + r, :, here] = top
                    sum_s[j * GROUP + r, :, here] = total

            return queries(j, r, b), parts, sink

        attend([block(b, r) for b in range(2 * OWN // BQ) for r in range(GROUP)])

    def far(j):
        def block(b, r):
            parts = [(key(n * CHUNK // OWN, j, n * CHUNK % OWN), value(n * CHUNK // OWN, j, n * CHUNK % OWN), False) for n in range(2 * OWN // CHUNK)]

            def sink(o, top, total):
                here = slice(b * BQ, (b + 1) * BQ)
                old = top_s[j * GROUP + r, :, here]
                new = jnp.maximum(old, top)
                a, c = jnp.exp2(old - new), jnp.exp2(top - new)
                finish(j, r, b, acc_s[j * GROUP + r, :, here] * a + o * c, sum_s[j * GROUP + r, :, here] * a + total * c)

            return queries(j, r, b), parts, sink

        attend([block(b, r) for b in range(2 * OWN // BQ) for r in range(GROUP)])

    def done(j):
        o_to_mate(j).start()

        @pl.when(j > 0)
        def _():
            close(j - 1)

        @pl.when((j > 0) & (j < HALF - 1))
        def _():
            for copy in wo_copies(j + 1):
                copy.start()

    @pl.when(chip == 0)
    def _():
        def step(j, _):
            near(j, True)
            done(j)

        lax.fori_loop(0, HALF, step, None)

    @pl.when(chip == 1)
    def _():
        lax.fori_loop(0, HALF, lambda j, _: near(j, False), None)

        def step(j, _):
            for n in range(2):
                remote(kst.at[0, 0], k_s.at[n, j], f_send.at[0, 0, 0], f_recv.at[0, n, j], 0).wait_recv()
                remote(vst.at[0, 0], v_s.at[n, j], f_send.at[1, 0, 0], f_recv.at[1, n, j], 0).wait_recv()
            far(j)
            done(j)

        lax.fori_loop(0, HALF, step, None)

    close(HALF - 1, last=True)
    for n in range(D // WIDE):
        y_copy(n).wait()

    @pl.when(chip == 0)
    def _():
        for owner in range(2):
            for j in range(HALF):
                k_across(owner, j).wait_send()
                v_across(owner, j).wait_send()


def attended(x, gain, wq, wk, wv, wo):
    dma = pltpu.SemaphoreType.DMA
    bf, f32 = jnp.bfloat16, jnp.float32
    anywhere = pl.BlockSpec(memory_space=pl.ANY)
    return pl.pallas_call(
        mixer,
        out_shape=jax.ShapeDtypeStruct((OWN, D), bf),
        in_specs=[anywhere, pl.BlockSpec(memory_space=pltpu.VMEM)] + [anywhere] * 5,
        out_specs=anywhere,
        scratch_shapes=[
            pltpu.VMEM((OWN, D), bf),
            pltpu.VMEM((SLOTS, D, WIDE), bf),
            pltpu.VMEM((OWN, 2 * HEAD), f32),
            pltpu.VMEM((2, HALF, OWN, HEAD), bf),
            pltpu.VMEM((2, HALF, HEAD, OWN), bf),
            pltpu.VMEM((3, MINE, OWN, HEAD), bf),
            pltpu.VMEM((4, HALF, OWN, HEAD), bf),
            pltpu.VMEM((4, HALF, HEAD, OWN), bf),
            pltpu.VMEM((RING, CHUNK, BQ), f32),
            pltpu.VMEM((MINE, HEAD, 2 * OWN), f32),
            pltpu.VMEM((MINE, 1, 2 * OWN), f32),
            pltpu.VMEM((MINE, 1, 2 * OWN), f32),
            pltpu.VMEM((2, HALF, OWN, 2 * GROUP * HEAD), bf),
            pltpu.VMEM((2, 2 * GROUP * HEAD, D), bf),
            pltpu.VMEM((OWN, D), f32),
            dma((2,)), dma((SLOTS, 2)), dma((2,)),
            dma((HALF,)), dma((HALF,)), dma((HALF,)), dma((HALF,)),
            dma((Q_TILES // 2,)), dma((Q_TILES // 2,)),
            dma((2, 2, HALF)), dma((2, 2, HALF)),
            dma((HALF,)), dma((HALF,)), dma((2, 2)), dma((D // WIDE,)),
        ],
        compiler_params=pltpu.CompilerParams(collective_id=0, has_side_effects=True, vmem_limit_bytes=60 * 2**20),
        cost_estimate=pl.CostEstimate(flops=40 * 10**9, bytes_accessed=60 * 2**20, transcendentals=20 * 10**6),
    )(x, gain, jnp.asarray(rope_table()), wq, wk, wv, wo)


def solution(mesh):
    def step(x, gain, wq, wk, wv, wo):
        return attended(x, gain, wq, wk, wv, wo)

    tokens, whole = P(("dp", "sp"), None), P(None, None)
    return jax.shard_map(
        step,
        mesh=mesh,
        in_specs=(tokens, P(None), whole, whole, whole, whole),
        out_specs=tokens,
        check_vma=False,
    )
```

```python
import functools

import jax
import jax.numpy as jnp
import numpy as np
from jax import lax
from jax.experimental import pallas as pl
from jax.experimental.pallas import tpu as pltpu
from jax.sharding import PartitionSpec as P

HEAD = 128
THETA = 10000
LOG2E = 1.4426950408889634
HIDDEN = -2e30
OWN = 512
D = 3072
KV = 8
HALF = 4
GROUP = 3
MINE = HALF * GROUP
WIDE = 512
Q_TILES = 6
SLOTS = 3
PARTS, PART = 4, 128
BQ = 256
CHUNK = 256
LEAD = 4
RING = 8


def dot(a, b, ca, cb):
    return lax.dot_general(a, b, (((ca,), (cb,)), ((), ())), preferred_element_type=jnp.float32)


def rope_table():
    half = HEAD // 2
    rate = np.float32(THETA) ** (-np.arange(half, dtype=np.float32) / np.float32(half))
    angle = np.arange(4 * OWN, dtype=np.float32)[:, None] * rate.astype(np.float32)
    return np.concatenate([np.cos(angle.astype(np.float64)), np.sin(angle.astype(np.float64))], -1).astype(np.float32)


def mixer(x_hbm, gain_ref, rope_hbm, wq, wk, wv, wo, y_hbm, a_s, w_s, rope_s, kst, vst, q_s, k_s, v_s, s_s, acc_s, top_s, sum_s, o_s, wo_s, y_s, raw_s,
          in_sem, w_sem, own_sem, k_send, k_recv, v_send, v_recv, q_send, q_recv, f_send, f_recv, o_send, o_recv, wo_sem, y_sem):
    me = lax.axis_index("sp")
    chip, core = lax.div(me, 2), lax.rem(me, 2)
    mate = 2 * chip + 1 - core
    e = HEAD**-0.5 * LOG2E

    def kv_copies(i, slot):
        col = pl.ds(pl.multiple_of(lax.rem(i, 2) * (HALF * HEAD) + lax.div(i, 2) * (WIDE // 2), WIDE // 2), WIDE // 2)
        return (pltpu.make_async_copy(wk.at[:, col], w_s.at[slot, :, : WIDE // 2], w_sem.at[slot, 0]),
                pltpu.make_async_copy(wv.at[:, col], w_s.at[slot, :, WIDE // 2 :], w_sem.at[slot, 1]))

    def q_copy(t, slot):
        col = pl.multiple_of(lax.rem(t + Q_TILES // 2 * (1 - core), Q_TILES) * WIDE, WIDE)
        return pltpu.make_async_copy(wq.at[:, pl.ds(col, WIDE)], w_s.at[slot], w_sem.at[slot, 0])

    def load_x(m):
        rows = slice(m * PART, (m + 1) * PART)
        return pltpu.make_async_copy(x_hbm.at[rows, :], a_s.at[rows, :], in_sem.at[m])

    load_rope = pltpu.make_async_copy(rope_hbm.at[pl.ds(pl.multiple_of(me * OWN, OWN), OWN), :], rope_s.at[:, :HEAD], in_sem.at[PARTS])
    load_rope.start()
    for m in range(PARTS):
        load_x(m).start()
    for copy in kv_copies(0, 0):
        copy.start()

    barrier = pltpu.get_barrier_semaphore()
    for step in (1, 2, 3):
        pl.semaphore_signal(barrier, inc=1, device_id={"sp": lax.rem(me + step, 4)}, device_id_type=pl.DeviceIdType.MESH)
    pl.semaphore_wait(barrier, 3)

    load_rope.wait()
    table = rope_s[:, :HEAD]
    swapped = pltpu.roll(table, HEAD // 2, 1)
    low = lax.broadcasted_iota(jnp.int32, (OWN, HEAD), 1) < HEAD // 2
    rope_s[:, :HEAD] = jnp.where(low, table, swapped)
    rope_s[:, HEAD:] = jnp.where(low, -swapped, table)
    gain = gain_ref[...].astype(jnp.float32)[None]

    def norm(m):
        for n in range(PART // 16):
            rows = slice(m * PART + n * 16, m * PART + (n + 1) * 16)
            wide = a_s[rows, :].astype(jnp.float32)
            y_s[rows, :] = wide
            scale = lax.rsqrt(jnp.mean(wide * wide, -1, keepdims=True) + 1e-6)
            a_s[rows, :] = (wide * scale * gain).astype(jnp.bfloat16)

    def turned(t, rows=slice(None)):
        t = t.astype(jnp.bfloat16).astype(jnp.float32)
        return (t * rope_s[rows, :HEAD] + pltpu.roll(t, HEAD // 2, 1) * rope_s[rows, HEAD:]).astype(jnp.bfloat16)

    def remote(src, dst, send, recv, to):
        return pltpu.make_async_remote_copy(src_ref=src, dst_ref=dst, send_sem=send, recv_sem=recv, device_id={"sp": to},
                                            device_id_type=pl.DeviceIdType.MESH)

    def k_to_mate(j):
        return remote(kst.at[1 - core, j], k_s.at[me, j], k_send.at[j], k_recv.at[j], mate)

    def v_to_mate(j):
        return remote(vst.at[1 - core, j], v_s.at[me, j], v_send.at[j], v_recv.at[j], mate)

    def k_across(owner, j):
        return remote(kst.at[owner, j], k_s.at[me, j], f_send.at[0, owner, j], f_recv.at[0, me, j], 2 + owner)

    def v_across(owner, j):
        return remote(vst.at[owner, j], v_s.at[me, j], f_send.at[1, owner, j], f_recv.at[1, me, j], 2 + owner)

    def load_tile(n):
        for copy in kv_copies(n, n % SLOTS) if n < 4 else (q_copy(n - 4, n % SLOTS),):
            copy.start()

    def kv_project(i, rows=slice(None)):
        return dot(a_s[rows, :], w_s[i % SLOTS], 1, 0)

    def kv_keep(i, kv, rows=slice(None)):
        owner, head = i % 2, 2 * (i // 2)
        for n in range(2):
            kst[owner, head + n, rows, :] = turned(kv[:, n * HEAD : (n + 1) * HEAD], rows)
            vst[owner, head + n, :, rows] = kv[:, (n + 2) * HEAD : (n + 3) * HEAD].astype(jnp.bfloat16).T

    def kv_send(i):
        owner, head = i % 2, 2 * (i // 2)

        @pl.when(chip == 0)
        def _():
            for to, j in ([(1, head), (0, head + 1), (1, head + 1)] if owner else [(0, head)]):
                k_across(to, j).start()
                v_across(to, j).start()

        @pl.when(core != owner)
        def _():
            for n in range(2):
                k_to_mate(head + n).start()
                v_to_mate(head + n).start()

    def kv_wait(i):
        for copy in kv_copies(i, i % SLOTS):
            copy.wait()

    load_x(0).wait()
    norm(0)
    for m in range(1, PARTS):
        load_x(m).wait()
    load_tile(1)
    kv_wait(0)
    load_tile(2)
    for m in range(PARTS):
        rows = slice(m * PART, (m + 1) * PART)
        kv = kv_project(0, rows)
        if m + 1 < PARTS:
            norm(m + 1)
        kv_keep(0, kv, rows)
    kv_send(0)
    load_tile(SLOTS)
    kv_wait(1)
    raw_s[...] = kv_project(1)
    load_tile(SLOTS + 1)
    for i in (2, 3):
        kv_wait(i)
        new = kv_project(i)
        kv_keep(i - 1, raw_s[...])
        raw_s[...] = new
        load_tile(SLOTS + i)
        kv_send(i - 1)

    def q_to_mate(t):
        four = pl.ds(4 * t, 4)
        return remote(q_s.at[0, four], q_s.at[1 + core, four], q_send.at[t], q_recv.at[t], mate)

    def q_project(t):
        slot = lax.rem(t + 4, SLOTS)
        q_copy(t, slot).wait()
        return dot(a_s[...], w_s[slot], 1, 0)

    def q_keep(t, q):
        away = t < Q_TILES // 2
        place, head = jnp.where(away, 0, 1 + core), 4 * jnp.where(away, t, t - Q_TILES // 2)
        for n in range(4):
            q_s[place, head + n] = turned(q[:, n * HEAD : (n + 1) * HEAD])

    new = q_project(0)
    kv_keep(3, raw_s[...])
    raw_s[...] = new
    q_copy(SLOTS, 4 % SLOTS).start()
    kv_send(3)
    own_k = pltpu.make_async_copy(kst.at[core], k_s.at[me], own_sem.at[0])
    own_v = pltpu.make_async_copy(vst.at[core], v_s.at[me], own_sem.at[1])
    own_k.start()
    own_v.start()

    def query(t, _):
        new = q_project(t)
        q_keep(t - 1, raw_s[...])
        raw_s[...] = new

        @pl.when(t < Q_TILES - SLOTS)
        def _():
            q_copy(t + SLOTS, lax.rem(t + 4, SLOTS)).start()

        @pl.when(t <= Q_TILES // 2)
        def _():
            q_to_mate(t - 1).start()

    lax.fori_loop(1, Q_TILES, query, None)
    q_keep(jnp.int32(Q_TILES - 1), raw_s[...])

    RUN = GROUP * HEAD

    def wo_copies(j):
        slot = lax.rem(j, 2)
        return tuple(pltpu.make_async_copy(wo.at[pl.ds(pl.multiple_of((owner * HALF + j) * RUN, RUN), RUN), :],
                                           wo_s.at[slot, n * RUN : (n + 1) * RUN], wo_sem.at[slot, n])
                     for n, owner in enumerate((core, 1 - core)))

    def y_copy(n):
        return pltpu.make_async_copy(a_s.at[:, n * WIDE : (n + 1) * WIDE], y_hbm.at[:, n * WIDE : (n + 1) * WIDE], y_sem.at[n])

    for j in range(2):
        for copy in wo_copies(j):
            copy.start()

    def close(j, last=False):
        for copy in wo_copies(j):
            copy.wait()
        o_to_mate(j).wait()
        slot = lax.rem(j, 2)
        for n in range(D // WIDE):
            here = slice(n * WIDE, (n + 1) * WIDE)
            y = y_s[:, here] + dot(o_s[core, j], wo_s[slot, :, here], 1, 0)
            if last:
                a_s[:, here] = y.astype(jnp.bfloat16)
                y_copy(n).start()
            else:
                y_s[:, here] = y

    own_k.wait()
    own_v.wait()
    for j in range(HALF):
        k_to_mate(j).wait()
        v_to_mate(j).wait()
    for t in range(Q_TILES // 2):
        q_to_mate(t).wait()

    def attend(blocks):
        chunks = [(i, n) for i, (_, parts, _) in enumerate(blocks) for n in range(len(parts))]
        tops = {}

        def score(g):
            if g >= len(chunks):
                return
            i, n = chunks[g]
            queries, parts, _ = blocks[i]
            keys, _, masked = parts[n]
            s = dot(keys(), queries(), 1, 1)
            if masked:
                s = jnp.where(lax.broadcasted_iota(jnp.int32, s.shape, 0) > lax.broadcasted_iota(jnp.int32, s.shape, 1), HIDDEN, s)
            s_s[g % RING] = s
            top = s.reshape(CHUNK // 8, 8, BQ).max(axis=0)
            tops[i] = jnp.maximum(tops[i], top) if i in tops else top

        for g in range(LEAD):
            score(g)
        g = 0
        for i, (_, parts, sink) in enumerate(blocks):
            top = tops[i].max(axis=0, keepdims=True) * e
            out = total = None
            for _, values, _ in parts:
                score(g + LEAD)
                p = jnp.exp2(s_s[g % RING] * e - top)
                t = p.reshape(CHUNK // 8, 8, BQ).sum(axis=0)
                o = dot(values(), p.astype(jnp.bfloat16), 1, 0)
                out, total = (o, t) if out is None else (out + o, total + t)
                g += 1
            sink(out, top, total.sum(axis=0, keepdims=True))

    def key(block, j, row):
        return lambda: k_s[block, j, row : row + CHUNK, :]

    def value(block, j, row):
        return lambda: v_s[block, j, :, row : row + CHUNK]

    def queries(j, r, b):
        return lambda: q_s[1 + b * BQ // OWN, j * GROUP + r, b * BQ % OWN : b * BQ % OWN + BQ, :]

    def o_to_mate(j):
        return remote(o_s.at[1 - core, j, :, :RUN], o_s.at[1 - core, j, :, RUN:], o_send.at[j], o_recv.at[j], mate)

    def finish(j, r, b, o, total):
        rows = b * BQ % OWN
        o_s[b * BQ // OWN, j, rows : rows + BQ, r * HEAD : (r + 1) * HEAD] = (o * (1 / total)).T.astype(jnp.bfloat16)

    def near(j, last):
        def block(b, r):
            parts = []
            for n in range(b + 1):
                at = 2 * chip + n * CHUNK // OWN, j, n * CHUNK % OWN
                parts.append((key(*at), value(*at), n == b))

            def sink(o, top, total):
                if last:
                    finish(j, r, b, o, total)
                else:
                    here = slice(b * BQ, (b + 1) * BQ)
                    acc_s[j * GROUP + r, :, here] = o
                    top_s[j * GROUP + r, :, here] = top
                    sum_s[j * GROUP + r, :, here] = total

            return queries(j, r, b), parts, sink

        attend([block(b, r) for b in range(2 * OWN // BQ) for r in range(GROUP)])

    def far(j):
        def block(b, r):
            parts = [(key(n * CHUNK // OWN, j, n * CHUNK % OWN), value(n * CHUNK // OWN, j, n * CHUNK % OWN), False) for n in range(2 * OWN // CHUNK)]

            def sink(o, top, total):
                here = slice(b * BQ, (b + 1) * BQ)
                old = top_s[j * GROUP + r, :, here]
                new = jnp.maximum(old, top)
                a, c = jnp.exp2(old - new), jnp.exp2(top - new)
                finish(j, r, b, acc_s[j * GROUP + r, :, here] * a + o * c, sum_s[j * GROUP + r, :, here] * a + total * c)

            return queries(j, r, b), parts, sink

        attend([block(b, r) for b in range(2 * OWN // BQ) for r in range(GROUP)])

    def done(j):
        o_to_mate(j).start()

        @pl.when(j > 0)
        def _():
            close(j - 1)

        @pl.when((j > 0) & (j < HALF - 1))
        def _():
            for copy in wo_copies(j + 1):
                copy.start()

    @pl.when(chip == 0)
    def _():
        def step(j, _):
            near(j, True)
            done(j)

        lax.fori_loop(0, HALF, step, None)

    @pl.when(chip == 1)
    def _():
        lax.fori_loop(0, HALF, lambda j, _: near(j, False), None)

        def step(j, _):
            for n in range(2):
                remote(kst.at[0, 0], k_s.at[n, j], f_send.at[0, 0, 0], f_recv.at[0, n, j], 0).wait_recv()
                remote(vst.at[0, 0], v_s.at[n, j], f_send.at[1, 0, 0], f_recv.at[1, n, j], 0).wait_recv()
            far(j)
            done(j)

        lax.fori_loop(0, HALF, step, None)

    close(HALF - 1, last=True)
    for n in range(D // WIDE):
        y_copy(n).wait()

    @pl.when(chip == 0)
    def _():
        for owner in range(2):
            for j in range(HALF):
                k_across(owner, j).wait_send()
                v_across(owner, j).wait_send()


def attended(x, gain, wq, wk, wv, wo):
    dma = pltpu.SemaphoreType.DMA
    bf, f32 = jnp.bfloat16, jnp.float32
    anywhere = pl.BlockSpec(memory_space=pl.ANY)
    return pl.pallas_call(
        mixer,
        out_shape=jax.ShapeDtypeStruct((OWN, D), bf),
        in_specs=[anywhere, pl.BlockSpec(memory_space=pltpu.VMEM)] + [anywhere] * 5,
        out_specs=anywhere,
        scratch_shapes=[
            pltpu.VMEM((OWN, D), bf),
            pltpu.VMEM((SLOTS, D, WIDE), bf),
            pltpu.VMEM((OWN, 2 * HEAD), f32),
            pltpu.VMEM((2, HALF, OWN, HEAD), bf),
            pltpu.VMEM((2, HALF, HEAD, OWN), bf),
            pltpu.VMEM((3, MINE, OWN, HEAD), bf),
            pltpu.VMEM((4, HALF, OWN, HEAD), bf),
            pltpu.VMEM((4, HALF, HEAD, OWN), bf),
            pltpu.VMEM((RING, CHUNK, BQ), f32),
            pltpu.VMEM((MINE, HEAD, 2 * OWN), f32),
            pltpu.VMEM((MINE, 1, 2 * OWN), f32),
            pltpu.VMEM((MINE, 1, 2 * OWN), f32),
            pltpu.VMEM((2, HALF, OWN, 2 * GROUP * HEAD), bf),
            pltpu.VMEM((2, 2 * GROUP * HEAD, D), bf),
            pltpu.VMEM((OWN, D), f32),
            pltpu.VMEM((OWN, WIDE), f32),
            dma((PARTS + 1,)), dma((SLOTS, 2)), dma((2,)),
            dma((HALF,)), dma((HALF,)), dma((HALF,)), dma((HALF,)),
            dma((Q_TILES // 2,)), dma((Q_TILES // 2,)),
            dma((2, 2, HALF)), dma((2, 2, HALF)),
            dma((HALF,)), dma((HALF,)), dma((2, 2)), dma((D // WIDE,)),
        ],
        compiler_params=pltpu.CompilerParams(collective_id=0, has_side_effects=True, vmem_limit_bytes=60 * 2**20),
        cost_estimate=pl.CostEstimate(flops=40 * 10**9, bytes_accessed=60 * 2**20, transcendentals=20 * 10**6),
    )(x, gain, jnp.asarray(rope_table()), wq, wk, wv, wo)


def solution(mesh):
    def step(x, gain, wq, wk, wv, wo):
        return attended(x, gain, wq, wk, wv, wo)

    tokens, whole = P(("dp", "sp"), None), P(None, None)
    return jax.shard_map(
        step,
        mesh=mesh,
        in_specs=(tokens, P(None), whole, whole, whole, whole),
        out_specs=tokens,
        check_vma=False,
    )
```

```python
import functools

import jax
import jax.numpy as jnp
import numpy as np
from jax import lax
from jax.experimental import pallas as pl
from jax.experimental.pallas import tpu as pltpu
from jax.sharding import PartitionSpec as P

HEAD = 128
THETA = 10000
LOG2E = 1.4426950408889634
HIDDEN = -2e30
OWN = 512
D = 3072
KV = 8
HALF = 4
GROUP = 3
MINE = HALF * GROUP
WIDE = 512
Q_TILES = 6
SLOTS = 3
PARTS, PART = 4, 128
BQ = 256
CHUNK = 256
LEAD = 4
RING = 8


def dot(a, b, ca, cb):
    return lax.dot_general(a, b, (((ca,), (cb,)), ((), ())), preferred_element_type=jnp.float32)


def rope_table():
    half = HEAD // 2
    rate = np.float32(THETA) ** (-np.arange(half, dtype=np.float32) / np.float32(half))
    angle = np.arange(4 * OWN, dtype=np.float32)[:, None] * rate.astype(np.float32)
    return np.concatenate([np.cos(angle.astype(np.float64)), np.sin(angle.astype(np.float64))], -1).astype(np.float32)


def mixer(x_hbm, gain_ref, rope_hbm, wq, wk, wv, wo, y_ref, a_s, w_s, rope_s, kst, vst, q_s, k_s, v_s, s_s, acc_s, top_s, sum_s, o_s, y_s, raw_s,
          in_sem, w_sem, own_sem, k_send, k_recv, v_send, v_recv, q_send, q_recv, f_send, f_recv, o_send, o_recv, wo_sem):
    me = lax.axis_index("sp")
    chip, core = lax.div(me, 2), lax.rem(me, 2)
    mate = 2 * chip + 1 - core
    e = HEAD**-0.5 * LOG2E

    def kv_copies(i, slot):
        col = pl.ds(pl.multiple_of(lax.rem(i, 2) * (HALF * HEAD) + lax.div(i, 2) * (WIDE // 2), WIDE // 2), WIDE // 2)
        return (pltpu.make_async_copy(wk.at[:, col], w_s.at[slot, :, : WIDE // 2], w_sem.at[slot, 0]),
                pltpu.make_async_copy(wv.at[:, col], w_s.at[slot, :, WIDE // 2 :], w_sem.at[slot, 1]))

    def q_copy(t, slot):
        col = pl.multiple_of(lax.rem(t + Q_TILES // 2 * (1 - core), Q_TILES) * WIDE, WIDE)
        return pltpu.make_async_copy(wq.at[:, pl.ds(col, WIDE)], w_s.at[slot], w_sem.at[slot, 0])

    def load_x(m):
        rows = slice(m * PART, (m + 1) * PART)
        return pltpu.make_async_copy(x_hbm.at[rows, :], a_s.at[rows, :], in_sem.at[m])

    load_rope = pltpu.make_async_copy(rope_hbm.at[pl.ds(pl.multiple_of(me * OWN, OWN), OWN), :], rope_s.at[:, :HEAD], in_sem.at[PARTS])
    load_rope.start()
    for m in range(PARTS):
        load_x(m).start()
    for copy in kv_copies(0, 0):
        copy.start()

    barrier = pltpu.get_barrier_semaphore()
    for step in (1, 2, 3):
        pl.semaphore_signal(barrier, inc=1, device_id={"sp": lax.rem(me + step, 4)}, device_id_type=pl.DeviceIdType.MESH)
    pl.semaphore_wait(barrier, 3)

    load_rope.wait()
    table = rope_s[:, :HEAD]
    swapped = pltpu.roll(table, HEAD // 2, 1)
    low = lax.broadcasted_iota(jnp.int32, (OWN, HEAD), 1) < HEAD // 2
    rope_s[:, :HEAD] = jnp.where(low, table, swapped)
    rope_s[:, HEAD:] = jnp.where(low, -swapped, table)
    gain = gain_ref[...].astype(jnp.float32)[None]

    def norm(m):
        for n in range(PART // 16):
            rows = slice(m * PART + n * 16, m * PART + (n + 1) * 16)
            wide = a_s[rows, :].astype(jnp.float32)
            y_s[rows, :] = wide
            scale = lax.rsqrt(jnp.mean(wide * wide, -1, keepdims=True) + 1e-6)
            a_s[rows, :] = (wide * scale * gain).astype(jnp.bfloat16)

    def turned(t, rows=slice(None)):
        t = t.astype(jnp.bfloat16).astype(jnp.float32)
        return (t * rope_s[rows, :HEAD] + pltpu.roll(t, HEAD // 2, 1) * rope_s[rows, HEAD:]).astype(jnp.bfloat16)

    def remote(src, dst, send, recv, to):
        return pltpu.make_async_remote_copy(src_ref=src, dst_ref=dst, send_sem=send, recv_sem=recv, device_id={"sp": to},
                                            device_id_type=pl.DeviceIdType.MESH)

    def k_to_mate(j):
        return remote(kst.at[1 - core, j], k_s.at[me, j], k_send.at[j], k_recv.at[j], mate)

    def v_to_mate(j):
        return remote(vst.at[1 - core, j], v_s.at[me, j], v_send.at[j], v_recv.at[j], mate)

    def k_across(owner, j):
        return remote(kst.at[owner, j], k_s.at[me, j], f_send.at[0, owner, j], f_recv.at[0, me, j], 2 + owner)

    def v_across(owner, j):
        return remote(vst.at[owner, j], v_s.at[me, j], f_send.at[1, owner, j], f_recv.at[1, me, j], 2 + owner)

    def load_tile(n):
        for copy in kv_copies(n, n % SLOTS) if n < 4 else (q_copy(n - 4, n % SLOTS),):
            copy.start()

    def kv_project(i, rows=slice(None)):
        return dot(a_s[rows, :], w_s[i % SLOTS], 1, 0)

    def kv_keep(i, kv, rows=slice(None)):
        owner, head = i % 2, 2 * (i // 2)
        for n in range(2):
            kst[owner, head + n, rows, :] = turned(kv[:, n * HEAD : (n + 1) * HEAD], rows)
            vst[owner, head + n, :, rows] = kv[:, (n + 2) * HEAD : (n + 3) * HEAD].astype(jnp.bfloat16).T

    def kv_send(i):
        owner, head = i % 2, 2 * (i // 2)

        @pl.when(chip == 0)
        def _():
            for to, j in ([(1, head), (0, head + 1), (1, head + 1)] if owner else [(0, head)]):
                k_across(to, j).start()
                v_across(to, j).start()

        @pl.when(core != owner)
        def _():
            for n in range(2):
                k_to_mate(head + n).start()
                v_to_mate(head + n).start()

    def kv_wait(i):
        for copy in kv_copies(i, i % SLOTS):
            copy.wait()

    load_x(0).wait()
    norm(0)
    for m in range(1, PARTS):
        load_x(m).wait()
    load_tile(1)
    kv_wait(0)
    load_tile(2)
    for m in range(PARTS):
        rows = slice(m * PART, (m + 1) * PART)
        kv = kv_project(0, rows)
        if m + 1 < PARTS:
            norm(m + 1)
        kv_keep(0, kv, rows)
    kv_send(0)
    load_tile(SLOTS)
    kv_wait(1)
    raw_s[...] = kv_project(1)
    load_tile(SLOTS + 1)
    for i in (2, 3):
        kv_wait(i)
        new = kv_project(i)
        kv_keep(i - 1, raw_s[...])
        raw_s[...] = new
        load_tile(SLOTS + i)
        kv_send(i - 1)

    def q_to_mate(t):
        four = pl.ds(4 * t, 4)
        return remote(q_s.at[0, four], q_s.at[1 + core, four], q_send.at[t], q_recv.at[t], mate)

    def q_project(t):
        slot = lax.rem(t + 4, SLOTS)
        q_copy(t, slot).wait()
        return dot(a_s[...], w_s[slot], 1, 0)

    def q_keep(t, q):
        away = t < Q_TILES // 2
        place, head = jnp.where(away, 0, 1 + core), 4 * jnp.where(away, t, t - Q_TILES // 2)
        for n in range(4):
            q_s[place, head + n] = turned(q[:, n * HEAD : (n + 1) * HEAD])

    new = q_project(0)
    kv_keep(3, raw_s[...])
    raw_s[...] = new
    q_copy(SLOTS, 4 % SLOTS).start()
    kv_send(3)
    own_k = pltpu.make_async_copy(kst.at[core], k_s.at[me], own_sem.at[0])
    own_v = pltpu.make_async_copy(vst.at[core], v_s.at[me], own_sem.at[1])
    own_k.start()
    own_v.start()

    def query(t, _):
        new = q_project(t)
        q_keep(t - 1, raw_s[...])
        raw_s[...] = new

        @pl.when(t < Q_TILES - SLOTS)
        def _():
            q_copy(t + SLOTS, lax.rem(t + 4, SLOTS)).start()

        @pl.when(t <= Q_TILES // 2)
        def _():
            q_to_mate(t - 1).start()

    lax.fori_loop(1, Q_TILES, query, None)
    q_keep(jnp.int32(Q_TILES - 1), raw_s[...])

    RUN = GROUP * HEAD

    def wo_place(j, n):
        at = lax.rem(j, 2) * (D // WIDE) + n
        return lax.div(at, 4), pl.multiple_of(lax.rem(at, 4) * (2 * RUN), 2 * RUN)

    def wo_copies(j, n):
        slot, row = wo_place(j, n)
        return [pltpu.make_async_copy(wo.at[pl.ds(pl.multiple_of((owner * HALF + j) * RUN, RUN), RUN), n * WIDE : (n + 1) * WIDE],
                                      w_s.at[slot, pl.ds(row + i * RUN, RUN), :], wo_sem.at[lax.rem(j, 2), n, i])
                for i, owner in enumerate((core, 1 - core))]

    def load_wo(j):
        for n in range(D // WIDE):
            for copy in wo_copies(j, n):
                copy.start()

    for j in range(2):
        load_wo(jnp.int32(j))

    def close(j, last=False):
        for n in range(D // WIDE):
            for copy in wo_copies(j, n):
                copy.wait()
        o_to_mate(j).wait()
        for n in range(D // WIDE):
            here = slice(n * WIDE, (n + 1) * WIDE)
            slot, row = wo_place(j, n)
            y = y_s[:, here] + dot(o_s[core, j], w_s[slot, pl.ds(row, 2 * RUN), :], 1, 0)
            if last:
                y_ref[:, here] = y.astype(jnp.bfloat16)
            else:
                y_s[:, here] = y

    own_k.wait()
    own_v.wait()
    for j in range(HALF):
        k_to_mate(j).wait()
        v_to_mate(j).wait()
    for t in range(Q_TILES // 2):
        q_to_mate(t).wait()

    def attend(blocks):
        chunks = [(i, n) for i, (_, parts, _) in enumerate(blocks) for n in range(len(parts))]
        tops = {}

        def score(g):
            if g >= len(chunks):
                return
            i, n = chunks[g]
            queries, parts, _ = blocks[i]
            keys, _, masked = parts[n]
            s = dot(keys(), queries(), 1, 1)
            if masked:
                s = jnp.where(lax.broadcasted_iota(jnp.int32, s.shape, 0) > lax.broadcasted_iota(jnp.int32, s.shape, 1), HIDDEN, s)
            s_s[g % RING] = s
            top = s.reshape(CHUNK // 8, 8, BQ).max(axis=0)
            tops[i] = jnp.maximum(tops[i], top) if i in tops else top

        for g in range(LEAD):
            score(g)
        g = 0
        for i, (_, parts, sink) in enumerate(blocks):
            top = tops[i].max(axis=0, keepdims=True)
            weights, total = [], None
            for _ in parts:
                score(g + LEAD)
                p = jnp.exp2((s_s[g % RING] - top) * e)
                t = p.reshape(CHUNK // 8, 8, BQ).sum(axis=0)
                total = t if total is None else total + t
                weights.append(p.astype(jnp.bfloat16))
                g += 1
            out = dot(jnp.concatenate([values() for _, values, _ in parts], axis=1), jnp.concatenate(weights, axis=0), 1, 0)
            sink(out, top, total.sum(axis=0, keepdims=True))

    def key(block, j, row):
        return lambda: k_s[block, j, row : row + CHUNK, :]

    def value(block, j, row):
        return lambda: v_s[block, j, :, row : row + CHUNK]

    def queries(j, r, b):
        return lambda: q_s[1 + b * BQ // OWN, j * GROUP + r, b * BQ % OWN : b * BQ % OWN + BQ, :]

    def o_to_mate(j):
        return remote(o_s.at[1 - core, j, :, :RUN], o_s.at[1 - core, j, :, RUN:], o_send.at[j], o_recv.at[j], mate)

    def finish(j, r, b, o, total):
        rows = b * BQ % OWN
        o_s[b * BQ // OWN, j, rows : rows + BQ, r * HEAD : (r + 1) * HEAD] = (o * (1 / total)).T.astype(jnp.bfloat16)

    def near(j, last):
        def block(b, r):
            parts = []
            for n in range(b + 1):
                at = 2 * chip + n * CHUNK // OWN, j, n * CHUNK % OWN
                parts.append((key(*at), value(*at), n == b))

            def sink(o, top, total):
                if last:
                    finish(j, r, b, o, total)
                else:
                    here = slice(b * BQ, (b + 1) * BQ)
                    acc_s[j * GROUP + r, :, here] = o
                    top_s[j * GROUP + r, :, here] = top
                    sum_s[j * GROUP + r, :, here] = total

            return queries(j, r, b), parts, sink

        attend([block(b, r) for b in range(2 * OWN // BQ) for r in range(GROUP)])

    def far(j):
        def block(b, r):
            parts = [(key(n * CHUNK // OWN, j, n * CHUNK % OWN), value(n * CHUNK // OWN, j, n * CHUNK % OWN), False) for n in range(2 * OWN // CHUNK)]

            def sink(o, top, total):
                here = slice(b * BQ, (b + 1) * BQ)
                old = top_s[j * GROUP + r, :, here]
                new = jnp.maximum(old, top)
                a, c = jnp.exp2((old - new) * e), jnp.exp2((top - new) * e)
                finish(j, r, b, acc_s[j * GROUP + r, :, here] * a + o * c, sum_s[j * GROUP + r, :, here] * a + total * c)

            return queries(j, r, b), parts, sink

        attend([block(b, r) for b in range(2 * OWN // BQ) for r in range(GROUP)])

    def done(j):
        o_to_mate(j).start()

        def one(i, _):
            close(i)

            @pl.when(i < HALF - 2)
            def _():
                load_wo(i + 2)

        lax.fori_loop(jnp.where(j < 2, 0, 1), jnp.where(j == 1, 1, jnp.where(j == 2, HALF - 1, 0)), one, None)

    @pl.when(chip == 0)
    def _():
        def step(j, _):
            near(j, True)
            done(j)

        lax.fori_loop(0, HALF, step, None)

    @pl.when(chip == 1)
    def _():
        lax.fori_loop(0, HALF, lambda j, _: near(j, False), None)

        def step(j, _):
            for n in range(2):
                remote(kst.at[0, 0], k_s.at[n, j], f_send.at[0, 0, 0], f_recv.at[0, n, j], 0).wait_recv()
                remote(vst.at[0, 0], v_s.at[n, j], f_send.at[1, 0, 0], f_recv.at[1, n, j], 0).wait_recv()
            far(j)
            done(j)

        lax.fori_loop(0, HALF, step, None)

    close(jnp.int32(HALF - 1), last=True)

    @pl.when(chip == 0)
    def _():
        for owner in range(2):
            for j in range(HALF):
                k_across(owner, j).wait_send()
                v_across(owner, j).wait_send()


def attended(x, gain, wq, wk, wv, wo):
    dma = pltpu.SemaphoreType.DMA
    bf, f32 = jnp.bfloat16, jnp.float32
    anywhere = pl.BlockSpec(memory_space=pl.ANY)
    return pl.pallas_call(
        mixer,
        out_shape=pltpu.VMEM((OWN, D), bf),
        in_specs=[anywhere, pl.BlockSpec(memory_space=pltpu.VMEM)] + [anywhere] * 5,
        out_specs=pl.BlockSpec(memory_space=pltpu.VMEM),
        scratch_shapes=[
            pltpu.VMEM((OWN, D), bf),
            pltpu.VMEM((SLOTS, D, WIDE), bf),
            pltpu.VMEM((OWN, 2 * HEAD), f32),
            pltpu.VMEM((2, HALF, OWN, HEAD), bf),
            pltpu.VMEM((2, HALF, HEAD, OWN), bf),
            pltpu.VMEM((3, MINE, OWN, HEAD), bf),
            pltpu.VMEM((4, HALF, OWN, HEAD), bf),
            pltpu.VMEM((4, HALF, HEAD, OWN), bf),
            pltpu.VMEM((RING, CHUNK, BQ), f32),
            pltpu.VMEM((MINE, HEAD, 2 * OWN), f32),
            pltpu.VMEM((MINE, 1, 2 * OWN), f32),
            pltpu.VMEM((MINE, 1, 2 * OWN), f32),
            pltpu.VMEM((2, HALF, OWN, 2 * GROUP * HEAD), bf),
            pltpu.VMEM((OWN, D), f32),
            pltpu.VMEM((OWN, WIDE), f32),
            dma((PARTS + 1,)), dma((SLOTS, 2)), dma((2,)),
            dma((HALF,)), dma((HALF,)), dma((HALF,)), dma((HALF,)),
            dma((Q_TILES // 2,)), dma((Q_TILES // 2,)),
            dma((2, 2, HALF)), dma((2, 2, HALF)),
            dma((HALF,)), dma((HALF,)), dma((2, D // WIDE, 2)),
        ],
        compiler_params=pltpu.CompilerParams(collective_id=0, has_side_effects=True, vmem_limit_bytes=56 * 2**20),
        cost_estimate=pl.CostEstimate(flops=40 * 10**9, bytes_accessed=60 * 2**20, transcendentals=20 * 10**6),
    )(x, gain, jnp.asarray(rope_table()), wq, wk, wv, wo)


def copying(y_in, y_ref, s2):
    outs = [pltpu.make_async_copy(y_in.at[n * 128 : (n + 1) * 128], y_ref.at[n * 128 : (n + 1) * 128], s2.at[n]) for n in range(4)]
    for o in outs:
        o.start()
    for o in outs:
        o.wait()


def copied(y):
    return pl.pallas_call(copying, out_shape=jax.ShapeDtypeStruct((OWN, D), jnp.bfloat16), in_specs=[pl.BlockSpec(memory_space=pltpu.VMEM)], out_specs=pl.BlockSpec(memory_space=pltpu.HBM),
        scratch_shapes=[pltpu.SemaphoreType.DMA((4,))],
        compiler_params=pltpu.CompilerParams(vmem_limit_bytes=5 * 2**20))(y)


def solution(mesh):
    def step(x, gain, wq, wk, wv, wo):
        return copied(attended(x, gain, wq, wk, wv, wo))

    tokens, whole = P(("dp", "sp"), None), P(None, None)
    return jax.shard_map(
        step,
        mesh=mesh,
        in_specs=(tokens, P(None), whole, whole, whole, whole),
        out_specs=tokens,
        check_vma=False,
    )
```

```python
import functools

import jax
import jax.numpy as jnp
import numpy as np
from jax import lax
from jax.experimental import pallas as pl
from jax.experimental.pallas import tpu as pltpu
from jax.sharding import PartitionSpec as P

HEAD = 128
THETA = 10000
LOG2E = 1.4426950408889634
HIDDEN = -2e30
OWN = 512
D = 3072
KV = 8
HALF = 4
GROUP = 3
MINE = HALF * GROUP
WIDE = 512
Q_TILES = 6
SLOTS = 3
PARTS, PART = 4, 128
BQ = 256
CHUNK = 256
LEAD = 4
RING = 8


def dot(a, b, ca, cb):
    return lax.dot_general(a, b, (((ca,), (cb,)), ((), ())), preferred_element_type=jnp.float32)


def rope_table():
    half = HEAD // 2
    rate = np.float32(THETA) ** (-np.arange(half, dtype=np.float32) / np.float32(half))
    angle = np.arange(4 * OWN, dtype=np.float32)[:, None] * rate.astype(np.float32)
    return np.concatenate([np.cos(angle.astype(np.float64)), np.sin(angle.astype(np.float64))], -1).astype(np.float32)


def mixer(x_hbm, gain_hbm, rope_hbm, wq, wk, wv, wo, y_ref, a_s, w_s, rope_s, kst, vst, q_s, k_s, v_s, s_s, acc_s, top_s, sum_s, o_s, y_s, raw_s, gain_s,
          in_sem, w_sem, own_sem, k_send, k_recv, v_send, v_recv, q_send, q_recv, f_send, f_recv, o_send, o_recv, wo_sem):
    me = lax.axis_index("sp")
    chip, core = lax.div(me, 2), lax.rem(me, 2)
    mate = 2 * chip + 1 - core
    e = HEAD**-0.5 * LOG2E

    def kv_copies(i, slot):
        col = pl.ds(pl.multiple_of(lax.rem(i, 2) * (HALF * HEAD) + lax.div(i, 2) * (WIDE // 2), WIDE // 2), WIDE // 2)
        return (pltpu.make_async_copy(wk.at[:, col], w_s.at[slot, :, : WIDE // 2], w_sem.at[slot, 0]),
                pltpu.make_async_copy(wv.at[:, col], w_s.at[slot, :, WIDE // 2 :], w_sem.at[slot, 1]))

    def q_copy(t, slot):
        col = pl.multiple_of(lax.rem(t + Q_TILES // 2 * (1 - core), Q_TILES) * WIDE, WIDE)
        return pltpu.make_async_copy(wq.at[:, pl.ds(col, WIDE)], w_s.at[slot], w_sem.at[slot, 0])

    def load_x(m):
        rows = slice(m * PART, (m + 1) * PART)
        return pltpu.make_async_copy(x_hbm.at[rows, :], a_s.at[rows, :], in_sem.at[m])

    load_rope = pltpu.make_async_copy(rope_hbm.at[pl.ds(pl.multiple_of(me * OWN, OWN), OWN), :], rope_s.at[:, :HEAD], in_sem.at[PARTS])
    load_gain = pltpu.make_async_copy(gain_hbm, gain_s, in_sem.at[PARTS + 1])
    load_gain.start()
    load_rope.start()
    for m in range(PARTS):
        load_x(m).start()
    for copy in kv_copies(0, 0):
        copy.start()

    barrier = pltpu.get_barrier_semaphore()
    for step in (1, 2, 3):
        pl.semaphore_signal(barrier, inc=1, device_id={"sp": lax.rem(me + step, 4)}, device_id_type=pl.DeviceIdType.MESH)

    load_rope.wait()
    table = rope_s[:, :HEAD]
    swapped = pltpu.roll(table, HEAD // 2, 1)
    low = lax.broadcasted_iota(jnp.int32, (OWN, HEAD), 1) < HEAD // 2
    rope_s[:, :HEAD] = jnp.where(low, table, swapped)
    rope_s[:, HEAD:] = jnp.where(low, -swapped, table)
    load_gain.wait()
    gain = gain_s[...].astype(jnp.float32)[None]

    def norm(m):
        for n in range(PART // 16):
            rows = slice(m * PART + n * 16, m * PART + (n + 1) * 16)
            wide = a_s[rows, :].astype(jnp.float32)
            y_s[rows, :] = wide
            scale = lax.rsqrt(jnp.mean(wide * wide, -1, keepdims=True) + 1e-6)
            a_s[rows, :] = (wide * scale * gain).astype(jnp.bfloat16)

    def turned(t, rows=slice(None)):
        t = t.astype(jnp.bfloat16).astype(jnp.float32)
        return (t * rope_s[rows, :HEAD] + pltpu.roll(t, HEAD // 2, 1) * rope_s[rows, HEAD:]).astype(jnp.bfloat16)

    def remote(src, dst, send, recv, to):
        return pltpu.make_async_remote_copy(src_ref=src, dst_ref=dst, send_sem=send, recv_sem=recv, device_id={"sp": to},
                                            device_id_type=pl.DeviceIdType.MESH)

    def k_to_mate(j):
        return remote(kst.at[1 - core, j], k_s.at[me, j], k_send.at[j], k_recv.at[j], mate)

    def v_to_mate(j):
        return remote(vst.at[1 - core, j], v_s.at[me, j], v_send.at[j], v_recv.at[j], mate)

    def k_across(owner, j):
        return remote(kst.at[owner, j], k_s.at[me, j], f_send.at[0, owner, j], f_recv.at[0, me, j], 2 + owner)

    def v_across(owner, j):
        return remote(vst.at[owner, j], v_s.at[me, j], f_send.at[1, owner, j], f_recv.at[1, me, j], 2 + owner)

    def load_tile(n):
        for copy in kv_copies(n, n % SLOTS) if n < 4 else (q_copy(n - 4, n % SLOTS),):
            copy.start()

    def kv_project(i, rows=slice(None)):
        return dot(a_s[rows, :], w_s[i % SLOTS], 1, 0)

    def kv_keep(i, kv, rows=slice(None)):
        owner, head = i % 2, 2 * (i // 2)
        for n in range(2):
            kst[owner, head + n, rows, :] = turned(kv[:, n * HEAD : (n + 1) * HEAD], rows)
            vst[owner, head + n, :, rows] = kv[:, (n + 2) * HEAD : (n + 3) * HEAD].astype(jnp.bfloat16).T

    def kv_send(i):
        owner, head = i % 2, 2 * (i // 2)

        @pl.when(chip == 0)
        def _():
            last = (core, 1 - core) if i == 3 else (0, 1)
            for to, j in ([(1, head), (last[0], head + 1), (last[1], head + 1)] if owner else [(0, head)]):
                k_across(to, j).start()
                v_across(to, j).start()

        @pl.when(core != owner)
        def _():
            for n in range(2):
                k_to_mate(head + n).start()
                v_to_mate(head + n).start()

    def kv_wait(i):
        for copy in kv_copies(i, i % SLOTS):
            copy.wait()

    load_x(0).wait()
    norm(0)
    for m in range(1, PARTS):
        load_x(m).wait()
    load_tile(1)
    kv_wait(0)
    load_tile(2)
    for m in range(PARTS):
        rows = slice(m * PART, (m + 1) * PART)
        kv = kv_project(0, rows)
        if m + 1 < PARTS:
            norm(m + 1)
        kv_keep(0, kv, rows)
    pl.semaphore_wait(barrier, 3)
    kv_send(0)
    load_tile(SLOTS)
    kv_wait(1)
    raw_s[...] = kv_project(1)
    load_tile(SLOTS + 1)
    for i in (2, 3):
        kv_wait(i)
        new = kv_project(i)
        kv_keep(i - 1, raw_s[...])
        raw_s[...] = new
        load_tile(SLOTS + i)
        kv_send(i - 1)

    def q_to_mate(t):
        four = pl.ds(4 * t, 4)
        return remote(q_s.at[0, four], q_s.at[1 + core, four], q_send.at[t], q_recv.at[t], mate)

    def q_project(t):
        slot = lax.rem(t + 4, SLOTS)
        q_copy(t, slot).wait()
        return dot(a_s[...], w_s[slot], 1, 0)

    def q_keep(t, q):
        away = t < Q_TILES // 2
        place, head = jnp.where(away, 0, 1 + core), 4 * jnp.where(away, t, t - Q_TILES // 2)
        for n in range(4):
            q_s[place, head + n] = turned(q[:, n * HEAD : (n + 1) * HEAD])

    new = q_project(0)
    kv_keep(3, raw_s[...])
    raw_s[...] = new
    q_copy(SLOTS, 4 % SLOTS).start()
    kv_send(3)
    own_k = pltpu.make_async_copy(kst.at[core], k_s.at[me], own_sem.at[0])
    own_v = pltpu.make_async_copy(vst.at[core], v_s.at[me], own_sem.at[1])
    own_k.start()
    own_v.start()

    def query(t, _):
        new = q_project(t)
        q_keep(t - 1, raw_s[...])
        raw_s[...] = new

        @pl.when(t < Q_TILES - SLOTS)
        def _():
            q_copy(t + SLOTS, lax.rem(t + 4, SLOTS)).start()

        @pl.when(t <= Q_TILES // 2)
        def _():
            q_to_mate(t - 1).start()

    lax.fori_loop(1, Q_TILES, query, None)
    q_keep(jnp.int32(Q_TILES - 1), raw_s[...])

    RUN = GROUP * HEAD

    def wo_place(j, n):
        at = lax.rem(j, 2) * (D // WIDE) + n
        return lax.div(at, 4), pl.multiple_of(lax.rem(at, 4) * (2 * RUN), 2 * RUN)

    def wo_copies(j, n):
        slot, row = wo_place(j, n)
        return [pltpu.make_async_copy(wo.at[pl.ds(pl.multiple_of((owner * HALF + j) * RUN, RUN), RUN), n * WIDE : (n + 1) * WIDE],
                                      w_s.at[slot, pl.ds(row + i * RUN, RUN), :], wo_sem.at[lax.rem(j, 2), n, i])
                for i, owner in enumerate((core, 1 - core))]

    def load_wo(j):
        for n in range(D // WIDE):
            for copy in wo_copies(j, n):
                copy.start()

    for j in range(2):
        load_wo(jnp.int32(j))

    def close(j, last=False):
        for n in range(D // WIDE):
            for copy in wo_copies(j, n):
                copy.wait()
        o_to_mate(j).wait()
        for n in range(D // WIDE):
            here = slice(n * WIDE, (n + 1) * WIDE)
            slot, row = wo_place(j, n)
            y = y_s[:, here] + dot(o_s[core, j], w_s[slot, pl.ds(row, 2 * RUN), :], 1, 0)
            if last:
                y_ref[:, here] = y.astype(jnp.bfloat16)
            else:
                y_s[:, here] = y

    own_k.wait()
    own_v.wait()
    for j in range(HALF):
        k_to_mate(j).wait()
        v_to_mate(j).wait()
    for t in range(Q_TILES // 2):
        q_to_mate(t).wait()

    def attend(blocks):
        chunks = [(i, n) for i, (_, parts, _) in enumerate(blocks) for n in range(len(parts))]
        tops = {}

        def score(g):
            if g >= len(chunks):
                return
            i, n = chunks[g]
            queries, parts, _ = blocks[i]
            keys, _, masked = parts[n]
            s = dot(keys(), queries(), 1, 1)
            if masked:
                s = jnp.where(lax.broadcasted_iota(jnp.int32, s.shape, 0) > lax.broadcasted_iota(jnp.int32, s.shape, 1), HIDDEN, s)
            s_s[g % RING] = s
            top = s.reshape(CHUNK // 8, 8, BQ).max(axis=0)
            tops[i] = jnp.maximum(tops[i], top) if i in tops else top

        for g in range(LEAD):
            score(g)
        g = 0
        for i, (_, parts, sink) in enumerate(blocks):
            top = tops[i].max(axis=0, keepdims=True)
            weights, total = [], None
            for _ in parts:
                score(g + LEAD)
                p = jnp.exp2((s_s[g % RING] - top) * e)
                t = p.reshape(CHUNK // 8, 8, BQ).sum(axis=0)
                total = t if total is None else total + t
                weights.append(p.astype(jnp.bfloat16))
                g += 1
            out = dot(jnp.concatenate([values() for _, values, _ in parts], axis=1), jnp.concatenate(weights, axis=0), 1, 0)
            sink(out, top, total.sum(axis=0, keepdims=True))

    def key(block, j, row):
        return lambda: k_s[block, j, row : row + CHUNK, :]

    def value(block, j, row):
        return lambda: v_s[block, j, :, row : row + CHUNK]

    def queries(j, r, b):
        return lambda: q_s[1 + b * BQ // OWN, j * GROUP + r, b * BQ % OWN : b * BQ % OWN + BQ, :]

    def o_to_mate(j):
        return remote(o_s.at[1 - core, j, :, :RUN], o_s.at[1 - core, j, :, RUN:], o_send.at[j], o_recv.at[j], mate)

    def finish(j, r, u, b, o, total):
        o_s[u, j, b * BQ : (b + 1) * BQ, r * HEAD : (r + 1) * HEAD] = (o * (1 / total)).astype(jnp.bfloat16).T

    def near(j, last):
        def block(b, r):
            parts = []
            for n in range(b + 1):
                at = 2 * chip + n * CHUNK // OWN, j, n * CHUNK % OWN
                parts.append((key(*at), value(*at), n == b))

            def sink(o, top, total):
                if last:
                    finish(j, r, b * BQ // OWN, b % (OWN // BQ), o, total)
                else:
                    here = slice(b * BQ, (b + 1) * BQ)
                    acc_s[j * GROUP + r, :, here] = o
                    top_s[j * GROUP + r, :, here] = top
                    sum_s[j * GROUP + r, :, here] = total

            return queries(j, r, b), parts, sink

        attend([block(b, r) for b in range(2 * OWN // BQ) for r in range(GROUP)])

    def far(j, halves, given, keep=False):
        def block(u, b, r):
            parts = [(key(n, j, row), value(n, j, row), False) for n in given for row in range(0, OWN, CHUNK)]
            head, here = j * GROUP + r, pl.ds(pl.multiple_of(u * OWN + b * BQ, BQ), BQ)

            def sink(o, top, total):
                old = top_s[head, :, here]
                new = jnp.maximum(old, top)
                a, c = jnp.exp2((old - new) * e), jnp.exp2((top - new) * e)
                o, total = acc_s[head, :, here] * a + o * c, sum_s[head, :, here] * a + total * c
                if keep:
                    acc_s[head, :, here] = o
                    top_s[head, :, here] = new
                    sum_s[head, :, here] = total
                else:
                    finish(j, r, u, b, o, total)

            return (lambda: q_s[1 + u, head, b * BQ : (b + 1) * BQ, :]), parts, sink

        attend([block(u, b, r) for u in halves for b in range(OWN // BQ) for r in range(GROUP)])

    def far_wait(j, n):
        remote(kst.at[0, 0], k_s.at[n, j], f_send.at[0, 0, 0], f_recv.at[0, n, j], 0).wait_recv()
        remote(vst.at[0, 0], v_s.at[n, j], f_send.at[1, 0, 0], f_recv.at[1, n, j], 0).wait_recv()

    def done(j):
        o_to_mate(j).start()

        def one(i, _):
            close(i)

            @pl.when(i < HALF - 2)
            def _():
                load_wo(i + 2)

        lax.fori_loop(jnp.where(j < 2, 0, 1), jnp.where(j == 1, 1, jnp.where(j == 2, HALF - 1, 0)), one, None)

    @pl.when(chip == 0)
    def _():
        def step(j, _):
            near(j, True)
            done(j)

        lax.fori_loop(0, HALF, step, None)

    @pl.when(chip == 1)
    def _():
        lax.fori_loop(0, HALF, lambda j, _: near(j, False), None)

        def step(j, _):
            for n in range(2):
                far_wait(j, n)
            far(j, (0, 1), (0, 1))
            done(j)

        lax.fori_loop(0, HALF - 1, step, None)
        final = HALF - 1
        far_wait(final, core)
        far(final, (0, 1), (core,), keep=True)
        far_wait(final, 1 - core)
        far(final, (1 - core,), (1 - core,))
        o_to_mate(final).start()
        far(final, (core,), (1 - core,))

    close(jnp.int32(HALF - 1), last=True)

    @pl.when(chip == 0)
    def _():
        for owner in range(2):
            for j in range(HALF):
                k_across(owner, j).wait_send()
                v_across(owner, j).wait_send()


def attended(x, gain, wq, wk, wv, wo):
    dma = pltpu.SemaphoreType.DMA
    bf, f32 = jnp.bfloat16, jnp.float32
    anywhere = pl.BlockSpec(memory_space=pl.ANY)
    return pl.pallas_call(
        mixer,
        out_shape=pltpu.VMEM((OWN, D), bf),
        in_specs=[anywhere] * 7,
        out_specs=pl.BlockSpec(memory_space=pltpu.VMEM),
        scratch_shapes=[
            pltpu.VMEM((OWN, D), bf),
            pltpu.VMEM((SLOTS, D, WIDE), bf),
            pltpu.VMEM((OWN, 2 * HEAD), f32),
            pltpu.VMEM((2, HALF, OWN, HEAD), bf),
            pltpu.VMEM((2, HALF, HEAD, OWN), bf),
            pltpu.VMEM((3, MINE, OWN, HEAD), bf),
            pltpu.VMEM((4, HALF, OWN, HEAD), bf),
            pltpu.VMEM((4, HALF, HEAD, OWN), bf),
            pltpu.VMEM((RING, CHUNK, BQ), f32),
            pltpu.VMEM((MINE, HEAD, 2 * OWN), f32),
            pltpu.VMEM((MINE, 1, 2 * OWN), f32),
            pltpu.VMEM((MINE, 1, 2 * OWN), f32),
            pltpu.VMEM((2, HALF, OWN, 2 * GROUP * HEAD), bf),
            pltpu.VMEM((OWN, D), f32),
            pltpu.VMEM((OWN, WIDE), f32),
            pltpu.VMEM((D,), bf),
            dma((PARTS + 2,)), dma((SLOTS, 2)), dma((2,)),
            dma((HALF,)), dma((HALF,)), dma((HALF,)), dma((HALF,)),
            dma((Q_TILES // 2,)), dma((Q_TILES // 2,)),
            dma((2, 2, HALF)), dma((2, 2, HALF)),
            dma((HALF,)), dma((HALF,)), dma((2, D // WIDE, 2)),
        ],
        compiler_params=pltpu.CompilerParams(collective_id=0, has_side_effects=True, vmem_limit_bytes=56 * 2**20),
        cost_estimate=pl.CostEstimate(flops=40 * 10**9, bytes_accessed=60 * 2**20, transcendentals=20 * 10**6),
    )(x, gain, jnp.asarray(rope_table()), wq, wk, wv, wo)


def copying(y_in, y_ref, s2):
    outs = [pltpu.make_async_copy(y_in.at[n * 128 : (n + 1) * 128], y_ref.at[n * 128 : (n + 1) * 128], s2.at[n]) for n in range(4)]
    for o in outs:
        o.start()
    for o in outs:
        o.wait()


def copied(y):
    return pl.pallas_call(copying, out_shape=jax.ShapeDtypeStruct((OWN, D), jnp.bfloat16), in_specs=[pl.BlockSpec(memory_space=pltpu.VMEM)], out_specs=pl.BlockSpec(memory_space=pltpu.HBM),
        scratch_shapes=[pltpu.SemaphoreType.DMA((4,))],
        compiler_params=pltpu.CompilerParams(vmem_limit_bytes=5 * 2**20))(y)


def solution(mesh):
    def step(x, gain, wq, wk, wv, wo):
        return copied(attended(x, gain, wq, wk, wv, wo))

    tokens, whole = P(("dp", "sp"), None), P(None, None)
    return jax.shard_map(
        step,
        mesh=mesh,
        in_specs=(tokens, P(None), whole, whole, whole, whole),
        out_specs=tokens,
        check_vma=False,
    )
```
